16 devices in a mesh: dp: 2 (over y, z), ep: 8 (over x, core).
Axes of the slice: x: 4, y: 2, z: 1, core: 2. Of those that a mesh axis runs over, the one named last changes fastest.
The devices are a block of a 4x4x8 slice.
Arguments:
- x_in: bfloat16 [2048, 2048], P(('dp', 'ep')), parts along dimension 0
- k_cache: bfloat16 [2048, 32, 4, 128], P(('dp', 'ep')), parts along dimension 0
- v_cache: bfloat16 [2048, 32, 4, 128], P(('dp', 'ep')), parts along dimension 0
- cache_len: int32 [2048], P(('dp', 'ep')), parts along dimension 0
- topk_idx: int32 [2048, 8], P(('dp', 'ep')), parts along dimension 0
- ln_attn: bfloat16 [2048], replicated
- w_q: bfloat16 [2048, 4096], replicated
- w_k: bfloat16 [2048, 512], replicated
- w_v: bfloat16 [2048, 512], replicated
- q_norm: bfloat16 [128], replicated
- k_norm: bfloat16 [128], replicated
- w_o: bfloat16 [4096, 2048], replicated
- ln_moe: bfloat16 [2048], replicated
- w_router: bfloat16 [2048, 128], replicated
- w_gate: bfloat16 [128, 2048, 768], P('ep')
- w_up: bfloat16 [128, 2048, 768], P('ep')
- w_down: bfloat16 [128, 768, 2048], P('ep')
Outputs:
- output 1: bfloat16 [2048, 2048], P(('dp', 'ep')), parts along dimension 0
- output 2: bfloat16 [2048, 32, 4, 128], P(('dp', 'ep')), parts along dimension 0
- output 3: bfloat16 [2048, 32, 4, 128], P(('dp', 'ep')), parts along dimension 0
There are 2 independent parts. The reference program is written for one: setup_inputs(seed, part) draws one part's arguments, and reference() takes and returns one part's arrays. A program takes and returns all parts, laid end to end along the dimension named above; an argument that names none is the same for every part.
All inputs are finite; a program needn't handle non-finite values.
Results may differ from the reference program's by a relative error of at most 0.0142757.
Values are sent between devices in bfloat16 or wider.
A program may use at most 768 MiB of HBM per device.

```python
import jax
import jax.numpy as jnp
import numpy as np
from jax import lax

HIDDEN = 2048
Q_HEADS = 32
KV_HEADS = 4
HEAD_DIM = 128
EXPERTS = 128
TOP_K = 8
EXPERT_FF = 768
B_DEV = 128
CACHE_LEN = 32
EP_SIZE = 8
BATCH = B_DEV * EP_SIZE
E_LOCAL = EXPERTS // EP_SIZE
ROPE_BASE = 1000000.0
NORM_EPS = 1e-6


def draw_layout(len_key, route_key, local_key):
    pair_count = B_DEV * TOP_K
    cap_rows = min(B_DEV, 2 * pair_count // EP_SIZE)
    n_hot = EP_SIZE // TOP_K
    n_cold = EP_SIZE - n_hot
    rest_rows = pair_count - n_hot * cap_rows
    base_rows = rest_rows // n_cold
    extra_rows = rest_rows - base_rows * n_cold
    row_counts = [cap_rows] * n_hot + [base_rows + 1] * extra_rows + [base_rows] * (n_cold - extra_rows)
    rank_table = np.repeat(np.arange(EP_SIZE), row_counts).reshape(TOP_K, B_DEV).T
    dev_keys = jax.random.split(route_key, EP_SIZE + 1)
    dev_perm = jax.random.permutation(dev_keys[0], EP_SIZE)
    row_perms = jax.vmap(lambda key_one: jax.random.permutation(key_one, B_DEV))(dev_keys[1:])
    dev_table = dev_perm[jnp.asarray(rank_table)]
    dev_all = dev_table[row_perms]
    local_ids = jax.random.randint(local_key, (EP_SIZE, B_DEV, TOP_K), 0, E_LOCAL)
    topk_idx = (dev_all * E_LOCAL + local_ids).reshape(BATCH, TOP_K).astype(jnp.int32)
    len_keys = jax.random.split(len_key, 3)
    shard_top = jax.random.randint(len_keys[0], (EP_SIZE, 1), CACHE_LEN // 4, CACHE_LEN)
    len_draw = jax.random.randint(len_keys[1], (EP_SIZE, B_DEV), 1, shard_top).reshape(BATCH)
    longest = jax.random.randint(len_keys[2], (), 0, BATCH)
    cache_len = jnp.where(jnp.arange(BATCH) == longest, CACHE_LEN - 1, len_draw).astype(jnp.int32)
    return cache_len, topk_idx


def setup_inputs(seed: int = 0, part: int = 0) -> dict:
    base_key = jax.random.key(seed)
    part_keys = jax.random.split(jax.random.fold_in(base_key, part), 6)
    shared_keys = jax.random.split(base_key, 14)
    q_width = Q_HEADS * HEAD_DIM
    kv_width = KV_HEADS * HEAD_DIM

    def normal_of(rand_key, arr_shape, scale_mul):
        return jax.random.normal(rand_key, arr_shape, jnp.float32) * scale_mul

    cache_len, topk_idx = draw_layout(part_keys[3], part_keys[4], part_keys[5])
    cache_shape = (BATCH, CACHE_LEN, KV_HEADS, HEAD_DIM)
    return {
        'x_in': normal_of(part_keys[0], (BATCH, HIDDEN), 1.0).astype(jnp.bfloat16),
        'k_cache': normal_of(part_keys[1], cache_shape, 1.5).astype(jnp.bfloat16),
        'v_cache': normal_of(part_keys[2], cache_shape, 1.0).astype(jnp.bfloat16),
        'cache_len': cache_len,
        'topk_idx': topk_idx,
        'ln_attn': (1.0 + normal_of(shared_keys[0], (HIDDEN,), 0.3)).astype(jnp.bfloat16),
        'w_q': normal_of(shared_keys[1], (HIDDEN, q_width), HIDDEN ** -0.5).astype(jnp.bfloat16),
        'w_k': normal_of(shared_keys[2], (HIDDEN, kv_width), HIDDEN ** -0.5).astype(jnp.bfloat16),
        'w_v': normal_of(shared_keys[3], (HIDDEN, kv_width), HIDDEN ** -0.5).astype(jnp.bfloat16),
        'q_norm': (2.0 + normal_of(shared_keys[4], (HEAD_DIM,), 0.4)).astype(jnp.bfloat16),
        'k_norm': (2.0 + normal_of(shared_keys[5], (HEAD_DIM,), 0.4)).astype(jnp.bfloat16),
        'w_o': normal_of(shared_keys[6], (q_width, HIDDEN), q_width ** -0.5).astype(jnp.bfloat16),
        'ln_moe': (1.0 + normal_of(shared_keys[7], (HIDDEN,), 0.3)).astype(jnp.bfloat16),
        'w_router': normal_of(shared_keys[8], (HIDDEN, EXPERTS), 1.5 * HIDDEN ** -0.5).astype(jnp.bfloat16),
        'w_gate': normal_of(shared_keys[9], (EXPERTS, HIDDEN, EXPERT_FF), HIDDEN ** -0.5).astype(jnp.bfloat16),
        'w_up': normal_of(shared_keys[10], (EXPERTS, HIDDEN, EXPERT_FF), HIDDEN ** -0.5).astype(jnp.bfloat16),
        'w_down': normal_of(shared_keys[11], (EXPERTS, EXPERT_FF, HIDDEN), 3.0 * EXPERT_FF ** -0.5).astype(jnp.bfloat16),
    }


def norm_scale(values, gain_vec):
    return values * lax.rsqrt(jnp.mean(values * values, axis=-1, keepdims=True) + NORM_EPS) * gain_vec.astype(jnp.float32)


def rotate_halves(values, positions):
    half_dim = values.shape[-1] // 2
    freq_vec = ROPE_BASE ** (-jnp.arange(half_dim, dtype=jnp.float32) * 2.0 / values.shape[-1])
    angles = positions.astype(jnp.float32)[:, None, None] * freq_vec
    cosine = jnp.cos(angles)
    sine_val = jnp.sin(angles)
    lo_half = values[..., :half_dim]
    hi_half = values[..., half_dim:]
    return jnp.concatenate([lo_half * cosine - hi_half * sine_val, hi_half * cosine + lo_half * sine_val], axis=-1)


def reference(x_in, k_cache, v_cache, cache_len, topk_idx, ln_attn, w_q, w_k, w_v, q_norm, k_norm, w_o, ln_moe, w_router, w_gate, w_up, w_down):
    resid_in = x_in.astype(jnp.float32)
    normed = norm_scale(resid_in, ln_attn).astype(jnp.bfloat16)
    q_proj = jnp.dot(normed, w_q, preferred_element_type=jnp.float32).reshape(BATCH, Q_HEADS, HEAD_DIM)
    k_proj = jnp.dot(normed, w_k, preferred_element_type=jnp.float32).reshape(BATCH, KV_HEADS, HEAD_DIM)
    v_new = jnp.dot(normed, w_v, preferred_element_type=jnp.float32).astype(jnp.bfloat16).reshape(BATCH, KV_HEADS, HEAD_DIM)
    q_rot = rotate_halves(norm_scale(q_proj, q_norm), cache_len).astype(jnp.bfloat16)
    k_new = rotate_halves(norm_scale(k_proj, k_norm), cache_len).astype(jnp.bfloat16)
    slot_ids = jnp.arange(CACHE_LEN)
    is_new = slot_ids[None, :, None, None] == cache_len[:, None, None, None]
    k_full = jnp.where(is_new, k_new[:, None], k_cache)
    v_full = jnp.where(is_new, v_new[:, None], v_cache)

    def one_token(args_tok):
        q_tok, k_tok, v_tok, len_tok = args_tok
        q_grp = q_tok.reshape(KV_HEADS, Q_HEADS // KV_HEADS, HEAD_DIM).astype(jnp.float32)
        scores = jnp.einsum('grd,sgd->grs', q_grp, k_tok.astype(jnp.float32)) * HEAD_DIM ** -0.5
        scores = jnp.where(slot_ids <= len_tok, scores, -1e30)
        attn_prob = jax.nn.softmax(scores, axis=-1).astype(jnp.bfloat16)
        mixed = jnp.einsum('grs,sgd->grd', attn_prob.astype(jnp.float32), v_tok.astype(jnp.float32))
        return mixed.astype(jnp.bfloat16).reshape(Q_HEADS * HEAD_DIM)

    attn_out = lax.map(one_token, (q_rot, k_full, v_full, cache_len))
    x_mid = (resid_in + jnp.dot(attn_out, w_o, preferred_element_type=jnp.float32)).astype(jnp.bfloat16)
    resid_mid = x_mid.astype(jnp.float32)
    h_moe = norm_scale(resid_mid, ln_moe).astype(jnp.bfloat16)
    logits = jnp.dot(h_moe, w_router, preferred_element_type=jnp.float32)
    route_prob = jax.nn.softmax(logits, axis=-1)
    picked = jnp.take_along_axis(route_prob, topk_idx, axis=1)
    gate_wts = picked / jnp.sum(picked, axis=1, keepdims=True)
    tok_rows = jnp.repeat(h_moe, TOP_K, axis=0)

    def one_pair(args_pair):
        row_vec, expert = args_pair
        row_mat = row_vec[None, :]
        gate_act = jnp.dot(row_mat, w_gate[expert], preferred_element_type=jnp.float32)
        up_act = jnp.dot(row_mat, w_up[expert], preferred_element_type=jnp.float32)
        hidden_act = (jax.nn.silu(gate_act) * up_act).astype(jnp.bfloat16)
        return jnp.dot(hidden_act, w_down[expert], preferred_element_type=jnp.float32).astype(jnp.bfloat16)[0]

    expert_out = lax.map(one_pair, (tok_rows, topk_idx.reshape(BATCH * TOP_K)))
    moe_out = jnp.sum(expert_out.reshape(BATCH, TOP_K, HIDDEN).astype(jnp.float32) * gate_wts[:, :, None], axis=1)
    x_out = (resid_mid + moe_out).astype(jnp.bfloat16)
    return x_out, k_full, v_full
```

```python
import functools

import jax
import jax.numpy as jnp
from jax import lax
from jax.experimental import pallas as pl
from jax.experimental.pallas import tpu as pltpu
from jax.sharding import PartitionSpec as P

ROPE_BASE = 1000000.0
NORM_EPS = 1e-6
MESH = pl.DeviceIdType.MESH
F32 = jnp.float32
BF16 = jnp.bfloat16
SEATS = 128
SPLIT = 4


def norm_scale(values, gain_vec):
    return values * lax.rsqrt(jnp.mean(values * values, axis=-1, keepdims=True) + NORM_EPS) * gain_vec.astype(jnp.float32)


def rotate_halves(values, positions):
    half_dim = values.shape[-1] // 2
    freq_vec = ROPE_BASE ** (-jnp.arange(half_dim, dtype=jnp.float32) * 2.0 / values.shape[-1])
    angles = positions.astype(jnp.float32)[:, None, None] * freq_vec
    cosine = jnp.cos(angles)
    sine_val = jnp.sin(angles)
    lo_half = values[..., :half_dim]
    hi_half = values[..., half_dim:]
    return jnp.concatenate([lo_half * cosine - hi_half * sine_val, hi_half * cosine + lo_half * sine_val], axis=-1)


def attend_block(x_in, k_cache, v_cache, cache_len, ln_attn, w_q, w_k, w_v, q_norm, k_norm, w_o):
    n_batch, n_slots, kv_heads, head_dim = k_cache.shape
    q_heads = w_q.shape[1] // head_dim
    resid_in = x_in.astype(jnp.float32)
    normed = norm_scale(resid_in, ln_attn).astype(jnp.bfloat16)
    q_proj = jnp.dot(normed, w_q, preferred_element_type=jnp.float32).reshape(n_batch, q_heads, head_dim)
    k_proj = jnp.dot(normed, w_k, preferred_element_type=jnp.float32).reshape(n_batch, kv_heads, head_dim)
    v_new = jnp.dot(normed, w_v, preferred_element_type=jnp.float32).astype(jnp.bfloat16).reshape(n_batch, kv_heads, head_dim)
    q_rot = rotate_halves(norm_scale(q_proj, q_norm), cache_len).astype(jnp.bfloat16).reshape(n_batch, kv_heads, q_heads // kv_heads, head_dim)
    k_new = rotate_halves(norm_scale(k_proj, k_norm), cache_len).astype(jnp.bfloat16)
    len_col = cache_len[:, None, None, None]
    is_new = lax.broadcasted_iota(jnp.int32, (1, n_slots, 1, 1), 1) == len_col
    k_full = jnp.where(is_new, k_new[:, None], k_cache)
    v_full = jnp.where(is_new, v_new[:, None], v_cache)
    scores = jnp.einsum('bgrd,bsgd->bgrs', q_rot, k_full, preferred_element_type=jnp.float32) * head_dim ** -0.5
    seen = lax.broadcasted_iota(jnp.int32, (1, 1, 1, n_slots), 3) <= len_col
    attn_prob = jax.nn.softmax(jnp.where(seen, scores, -1e30), axis=-1).astype(jnp.bfloat16)
    attn_out = jnp.einsum('bgrs,bsgd->bgrd', attn_prob, v_full, preferred_element_type=jnp.float32).astype(jnp.bfloat16).reshape(n_batch, q_heads * head_dim)
    x_mid = (resid_in + jnp.dot(attn_out, w_o, preferred_element_type=jnp.float32)).astype(jnp.bfloat16)
    return x_mid, k_full, v_full


def route_gate(x_mid, ln_moe, w_router, topk_idx):
    resid_mid = x_mid.astype(jnp.float32)
    h_moe = norm_scale(resid_mid, ln_moe).astype(jnp.bfloat16)
    logits = jnp.dot(h_moe, w_router, preferred_element_type=jnp.float32)
    gate_wts = jax.nn.softmax(jnp.take_along_axis(logits, topk_idx, axis=1), axis=-1)
    return h_moe, gate_wts


def moe_kernel(ep_size, h_ref, x_ref, meta_ref, wg_hbm, wu_hbm, wd_hbm, out_ref, flag_ref,
               xall, mall, perm, keys, keyt, xg, hid, ys, ybuf, yrecv, zsum, recv1, recv2, fin,
               wg, wu, wd, s_w, s_d, s_own, s_fwd, s_pair, r_x, s_meta, r_meta,
               s_y, r_y, s_1, r_1, s_2, r_2, s_f, r_f):
    b_dev, hidden = h_ref.shape
    e_local, _, ff = wg_hbm.shape
    n_chip = ep_size // 2
    half = b_dev // 2
    wide = hidden // SPLIT
    side = wide // 2
    n_a, n_b = wg.shape[0], wd.shape[0]
    per = wd.shape[1]
    groups = e_local // per
    me = lax.axis_index('ep')
    chip, core = me // 2, me % 2
    right = lax.rem(chip + 1, n_chip)
    left = lax.rem(chip + n_chip - 1, n_chip)
    far = lax.rem(chip + 2, n_chip)
    dev_r, dev_l, mate = right * 2 + core, left * 2 + core, chip * 2 + 1 - core

    def load_a(e):
        slot = lax.rem(e, n_a)
        return (pltpu.make_async_copy(wg_hbm.at[e], wg.at[slot], s_w.at[0, slot]),
                pltpu.make_async_copy(wu_hbm.at[e], wu.at[slot], s_w.at[1, slot]))

    def load_b(i):
        slot = lax.rem(i, n_b)
        q, g = i // groups, lax.rem(i, groups)
        cols = pl.ds(pl.multiple_of(q * wide, wide), wide)
        return pltpu.make_async_copy(wd_hbm.at[pl.ds(g * per, per), :, cols], wd.at[slot], s_d.at[slot])

    for e in range(n_a):
        for c in load_a(e):
            c.start()
    for i in range(n_b):
        load_b(i).start()

    barrier = pltpu.get_barrier_semaphore()
    for k in range(1, ep_size):
        pl.semaphore_signal(barrier, inc=1, device_id={'ep': lax.rem(me + k, ep_size)}, device_id_type=MESH)
    pl.semaphore_wait(barrier, ep_size - 1)

    def part(h):
        return pl.ds(h * half, half)

    def send_own(h, target, sem):
        return pltpu.make_async_remote_copy(h_ref.at[part(h)], xall.at[me, part(h)], sem, r_x.at[me, h],
                                            device_id={'ep': target}, device_id_type=MESH)

    def forward(src, h, target, sem):
        return pltpu.make_async_remote_copy(xall.at[src, part(h)], xall.at[src, part(h)], sem, r_x.at[src, h],
                                            device_id={'ep': target}, device_id_type=MESH)

    def send_meta(k):
        return pltpu.make_async_remote_copy(meta_ref, mall.at[me], s_meta.at[k - 1], r_meta.at[me],
                                            device_id={'ep': lax.rem(me + k, ep_size)}, device_id_type=MESH)

    started = []

    def go(copy):
        copy.start()
        started.append(copy)

    for k in range(1, ep_size):
        go(send_meta(k))
    go(send_own(0, dev_r, s_own.at[0]))
    go(send_own(1, dev_l, s_own.at[1]))
    go(send_own(1, dev_r, s_own.at[2]))
    go(send_own(0, dev_l, s_own.at[3]))
    go(send_own(0, mate, s_own.at[4]))
    go(send_own(1, mate, s_own.at[5]))
    xall[me] = h_ref[...]
    mall[me] = meta_ref[...]

    forward(dev_l, 0, dev_r, s_fwd.at[0]).wait_recv()
    go(forward(dev_l, 0, dev_r, s_fwd.at[0]))
    go(forward(dev_l, 0, mate, s_pair.at[0]))
    forward(dev_r, 1, dev_l, s_fwd.at[1]).wait_recv()
    go(forward(dev_r, 1, dev_l, s_fwd.at[1]))
    go(forward(dev_r, 1, mate, s_pair.at[1]))

    for k in range(1, ep_size):
        src = lax.rem(me + k, ep_size)
        pltpu.make_async_remote_copy(meta_ref, mall.at[src], s_meta.at[k - 1], r_meta.at[src],
                                     device_id={'ep': src}, device_id_type=MESH).wait_recv()
    lower = lax.broadcasted_iota(jnp.int32, (b_dev, b_dev), 0) < lax.broadcasted_iota(jnp.int32, (b_dev, b_dev), 1)
    before = jnp.where(lower, 1.0, 0.0).astype(BF16)
    ids16 = lax.broadcasted_iota(jnp.int32, (e_local, b_dev), 0).astype(F32)
    keys[...] = jnp.zeros_like(keys)
    counts = jnp.zeros((e_local, 1), F32)
    for src in range(ep_size):
        row = mall[src, pl.ds(me, 1), :]
        hot = jnp.where(ids16 == row, 1.0, 0.0)
        ranks = jnp.dot(hot.astype(BF16), before, preferred_element_type=F32) + counts
        rank = jnp.sum(hot * ranks, axis=0, keepdims=True)
        keys[pl.ds(src, 1), :] = row * SEATS + rank
        keys[pl.ds(ep_size + src, 1), :] = mall[src, pl.ds(ep_size + me, 1), :]
        keys[pl.ds(2 * ep_size + src, 1), :] = mall[src, pl.ds(ep_size + mate, 1), :]
        counts = counts + jnp.sum(hot, axis=1, keepdims=True)
    keyt[...] = jnp.transpose(keys[...])
    most = jnp.zeros((e_local, 1), F32)
    for dev in range(ep_size):
        total = jnp.zeros((e_local, 1), F32)
        for src in range(ep_size):
            hot = jnp.where(ids16 == mall[src, pl.ds(dev, 1), :], 1.0, 0.0)
            total = total + jnp.sum(hot, axis=1, keepdims=True)
        most = jnp.maximum(most, total)
    flag_ref[...] = jnp.broadcast_to(jnp.max(most, axis=0, keepdims=True), flag_ref.shape)

    seat_cols = lax.broadcasted_iota(jnp.int32, (b_dev, 4 * SEATS), 1).astype(F32)
    for b in range(ep_size):
        col = keyt[:, b:b + 1]

        @pl.loop(0, e_local // 4)
        def _(j):
            base = (j * (4 * SEATS)).astype(F32)
            hot = jnp.where(seat_cols + base == col, 1.0, 0.0).astype(BF16)
            perm[b * b_dev:(b + 1) * b_dev, pl.ds(pl.multiple_of(j * (4 * SEATS), 4 * SEATS), 4 * SEATS)] = hot

    for src, h, sem in ((dev_l, 1, 2), (dev_r, 0, 3)):
        forward(src, h, mate, s_pair.at[sem]).wait_recv()
        go(forward(src, h, mate, s_pair.at[sem]))
    dev_f = far * 2 + core
    for h in range(2):
        forward(dev_f, h, mate, s_pair.at[4 + h]).wait_recv()
        go(forward(dev_f, h, mate, s_pair.at[4 + h]))
    for k in range(n_chip):
        src = lax.rem(chip + k, n_chip) * 2 + 1 - core
        for h in range(2):
            forward(src, h, mate, s_pair.at[h]).wait_recv()

    seat_rows = lax.broadcasted_iota(jnp.int32, (SEATS, b_dev), 0).astype(F32)

    @pl.loop(0, e_local)
    def _(e):
        slot = lax.rem(e, n_a)
        base = (e * SEATS).astype(F32)
        pick = jnp.concatenate(
            [jnp.where(keys[b:b + 1, :] == seat_rows + base, 1.0, 0.0).astype(BF16) for b in range(ep_size)], axis=1)
        for n in range(4):
            cols = slice(n * (hidden // 4), (n + 1) * (hidden // 4))
            rows = xall[:, :, cols].reshape(ep_size * b_dev, hidden // 4)
            xg[:, cols] = jnp.dot(pick, rows, preferred_element_type=F32).astype(BF16)
        for c in load_a(e):
            c.wait()
        for n in range(ff // 256):
            cols = slice(n * 256, (n + 1) * 256)
            gate = jnp.dot(xg[...], wg[slot, :, cols], preferred_element_type=F32)
            up = jnp.dot(xg[...], wu[slot, :, cols], preferred_element_type=F32)
            hid[e, :, cols] = (gate * jax.nn.sigmoid(gate) * up).astype(BF16)

        @pl.when(e + n_a < e_local)
        def _():
            for c in load_a(e + n_a):
                c.start()

    def send_y(q):
        return pltpu.make_async_remote_copy(ybuf.at[q, 1 - core], yrecv.at[q], s_y.at[q], r_y.at[q],
                                            device_id={'ep': mate}, device_id_type=MESH)

    def send_1(q, d):
        block = far * 2 + d
        return pltpu.make_async_remote_copy(zsum.at[q, block], recv1.at[d, q], s_1.at[d, q], r_1.at[d, q],
                                            device_id={'ep': dev_l if d else dev_r}, device_id_type=MESH)

    def send_2(q, d):
        block = (left if d else right) * 2
        return pltpu.make_async_remote_copy(zsum.at[q, pl.ds(block, 2)], recv2.at[d, q], s_2.at[d, q], r_2.at[d, q],
                                            device_id={'ep': dev_l if d else dev_r}, device_id_type=MESH)

    def send_f(q):
        return pltpu.make_async_remote_copy(zsum.at[q, mate], fin.at[q], s_f.at[q], r_f.at[q],
                                            device_id={'ep': mate}, device_id_type=MESH)

    def relay(q):
        for d in range(2):
            send_1(q, d).wait_recv()
            block = (left if d else right) * 2 + d
            zsum[q, block] = zsum[q, block] + recv1[d, q]
            send_2(q, d).start()

    @pl.loop(0, SPLIT)
    def _(q):
        @pl.loop(0, groups)
        def _(g):
            i = q * groups + g
            slot = lax.rem(i, n_b)
            load_b(i).wait()
            for j in range(per):
                e = g * per + j
                ys[pl.ds(pl.multiple_of(e * SEATS, SEATS), SEATS), :] = jnp.dot(
                    hid[e], wd[slot, j], preferred_element_type=F32).astype(BF16)

            @pl.when(i + n_b < SPLIT * groups)
            def _():
                load_b(i + n_b).start()

        @pl.loop(0, ep_size // 2)
        def _(m):
            rows = pl.ds(pl.multiple_of(m * (2 * b_dev), 2 * b_dev), 2 * b_dev)
            for h in range(2):
                part_y = jnp.dot(perm[rows, :], ys[:, h * side:(h + 1) * side], preferred_element_type=F32)
                ybuf[q, h, pl.ds(2 * m, 2)] = part_y.astype(BF16).reshape(2, b_dev, side)

        send_y(q).start()

        @pl.when(q > 0)
        def _():
            relay(q - 1)

        send_y(q).wait_recv()
        for b in range(ep_size):
            zsum[q, b] = (keyt[:, ep_size + b:ep_size + b + 1] * ybuf[q, core, b].astype(F32)
                          + keyt[:, 2 * ep_size + b:2 * ep_size + b + 1] * yrecv[q, b].astype(F32))
        send_1(q, 0).start()
        send_1(q, 1).start()

    relay(SPLIT - 1)

    def columns(q, which):
        return pl.ds(pl.multiple_of(q * wide + which * side, side), side)

    @pl.loop(0, SPLIT)
    def _(q):
        send_2(q, 0).wait_recv()
        send_2(q, 1).wait_recv()
        zsum[q, mate] = zsum[q, mate] + recv2[0, q, 1 - core] + recv2[1, q, 1 - core]
        send_f(q).start()
        mine = zsum[q, me] + recv2[0, q, core] + recv2[1, q, core]
        cols = columns(q, core)
        out_ref[:, cols] = (x_ref[:, cols].astype(F32) + mine).astype(BF16)

    @pl.loop(0, SPLIT)
    def _(q):
        send_f(q).wait_recv()
        cols = columns(q, 1 - core)
        out_ref[:, cols] = (x_ref[:, cols].astype(F32) + fin[q]).astype(BF16)

    for copy in started:
        copy.wait_send()

    @pl.loop(0, SPLIT)
    def _(q):
        send_y(q).wait_send()
        send_f(q).wait_send()
        for d in range(2):
            send_1(q, d).wait_send()
            send_2(q, d).wait_send()


def moe_block(ep_size, h_moe, x_mid, meta, w_gate, w_up, w_down):
    b_dev, hidden = h_moe.shape
    e_local, _, ff = w_gate.shape
    wide, side = hidden // SPLIT, hidden // SPLIT // 2
    n_a, n_b, per = 3, 4, 4
    vmem, dma = pltpu.VMEM, pltpu.SemaphoreType.DMA
    tokens = ep_size * b_dev
    return pl.pallas_call(
        functools.partial(moe_kernel, ep_size),
        out_shape=(jax.ShapeDtypeStruct((b_dev, hidden), BF16), jax.ShapeDtypeStruct((8, 128), F32)),
        in_specs=[pl.BlockSpec(memory_space=pltpu.VMEM)] * 3 + [pl.BlockSpec(memory_space=pl.ANY)] * 3,
        out_specs=(pl.BlockSpec(memory_space=pltpu.VMEM), pl.BlockSpec(memory_space=pltpu.VMEM)),
        scratch_shapes=[
            vmem((ep_size, b_dev, hidden), BF16), vmem((ep_size, 2 * ep_size, b_dev), F32),
            vmem((tokens, e_local * SEATS), BF16), vmem((b_dev, b_dev), F32), vmem((b_dev, b_dev), F32),
            vmem((SEATS, hidden), BF16), vmem((e_local, SEATS, ff), BF16), vmem((e_local * SEATS, wide), BF16),
            vmem((SPLIT, 2, ep_size, b_dev, side), BF16), vmem((SPLIT, ep_size, b_dev, side), BF16),
            vmem((SPLIT, ep_size, b_dev, side), F32), vmem((2, SPLIT, b_dev, side), F32),
            vmem((2, SPLIT, 2, b_dev, side), F32), vmem((SPLIT, b_dev, side), F32),
            vmem((n_a, hidden, ff), BF16), vmem((n_a, hidden, ff), BF16), vmem((n_b, per, ff, wide), BF16),
            dma((2, n_a)), dma((n_b,)), dma((6,)), dma((2,)), dma((6,)), dma((ep_size, 2)),
            dma((ep_size - 1,)), dma((ep_size,)),
            dma((SPLIT,)), dma((SPLIT,)), dma((2, SPLIT)), dma((2, SPLIT)), dma((2, SPLIT)), dma((2, SPLIT)),
            dma((SPLIT,)), dma((SPLIT,)),
        ],
        compiler_params=pltpu.CompilerParams(collective_id=0, has_side_effects=True, vmem_limit_bytes=67043328),
        name='moe',
    )(h_moe, x_mid, meta, w_gate, w_up, w_down)


def moe_general(ep_size, h_moe, x_mid, topk_idx, gate_wts, w_gate, w_up, w_down):
    b_dev, hidden = h_moe.shape
    e_local = w_gate.shape[0]
    owner = topk_idx // e_local
    hot = owner[:, None, :] == jnp.arange(ep_size)[None, :, None]
    local = jnp.sum(jnp.where(hot, (topk_idx % e_local)[:, None, :], 0), axis=2).T
    wts = jnp.sum(jnp.where(hot, gate_wts[:, None, :], 0.0), axis=2)
    rows = lax.all_to_all(jnp.broadcast_to(h_moe[None], (ep_size, b_dev, hidden)), 'ep', 0, 0, tiled=True)
    rows = rows.reshape(ep_size * b_dev, hidden)
    ids = lax.all_to_all(local[:, None, :], 'ep', 0, 0, tiled=True).reshape(ep_size * b_dev)

    def one(e, done):
        gate = jnp.dot(rows, w_gate[e], preferred_element_type=F32)
        up = jnp.dot(rows, w_up[e], preferred_element_type=F32)
        act = (jax.nn.silu(gate) * up).astype(BF16)
        y = jnp.dot(act, w_down[e], preferred_element_type=F32).astype(BF16)
        return jnp.where((ids == e)[:, None], y, done)

    y = lax.fori_loop(0, e_local, one, jnp.zeros(rows.shape, BF16))
    back = lax.all_to_all(y.reshape(ep_size, b_dev, hidden), 'ep', 0, 0, tiled=True)
    total = jnp.sum(back.astype(F32) * wts.T[:, :, None], axis=0)
    return (x_mid.astype(F32) + total).astype(BF16)


def solution(mesh):
    ep_size = mesh.shape['ep']
    row_spec = P(('dp', 'ep'))
    replicated = P()
    expert_spec = P('ep')
    in_specs = (row_spec,) * 5 + (replicated,) * 9 + (expert_spec,) * 3
    out_specs = (row_spec, row_spec, row_spec)

    def device_step(x_in, k_cache, v_cache, cache_len, topk_idx, ln_attn, w_q, w_k, w_v, q_norm, k_norm, w_o, ln_moe, w_router, w_gate, w_up, w_down):
        x_mid, k_full, v_full = attend_block(x_in, k_cache, v_cache, cache_len, ln_attn, w_q, w_k, w_v, q_norm, k_norm, w_o)
        h_moe, gate_wts = route_gate(x_mid, ln_moe, w_router, topk_idx)
        e_local = w_gate.shape[0]
        owner = topk_idx // e_local
        hot = owner[:, None, :] == jnp.arange(ep_size)[None, :, None]
        local = jnp.sum(jnp.where(hot, (topk_idx % e_local)[:, None, :], 0), axis=2).astype(F32)
        wts = jnp.sum(jnp.where(hot, gate_wts[:, None, :], 0.0), axis=2)
        meta = jnp.concatenate([local, wts], axis=1).T
        fast, most = moe_block(ep_size, h_moe, x_mid, meta, w_gate, w_up, w_down)
        x_out = lax.cond(most[0, 0] > SEATS,
                         lambda: moe_general(ep_size, h_moe, x_mid, topk_idx, gate_wts, w_gate, w_up, w_down),
                         lambda: fast)
        return x_out, k_full, v_full

    return jax.shard_map(device_step, mesh=mesh, in_specs=in_specs, out_specs=out_specs, check_vma=False)
```

```python
import functools

import jax
import jax.numpy as jnp
from jax import lax
from jax.experimental import pallas as pl
from jax.experimental.pallas import tpu as pltpu
from jax.sharding import PartitionSpec as P

ROPE_BASE = 1000000.0
NORM_EPS = 1e-6
MESH = pl.DeviceIdType.MESH
F32 = jnp.float32
BF16 = jnp.bfloat16
SEATS = 128
SPLIT = 4


def rms(values, gain):
    return values * lax.rsqrt(jnp.mean(values * values, axis=-1, keepdims=True) + NORM_EPS) * gain


def attend_kernel(ep_size, len_ref, x_ref, cos_ref, sin_ref, idx_ref, lna_ref, qn_ref, kn_ref, lnm_ref,
                  wq_hbm, wk_hbm, wv_hbm, wo_hbm, wr_hbm, kc_hbm, vc_hbm,
                  xmid_ref, h_ref, meta_ref, ko_hbm, vo_hbm,
                  wq, wk, wv, wo, wr, kbuf, vbuf, qs, os, knew, vnew, hn, att,
                  s_q, s_kv, s_o, s_c, s_out):
    b_dev, hidden = x_ref.shape
    _, lanes, dim = kbuf.shape
    q_width = wq.shape[1]
    q_heads, kv_heads = q_width // dim, wk.shape[1] // dim
    n_q, n_o = s_q.shape[0], s_o.shape[0]
    n_blk = s_c.shape[1]
    blk = b_dev // n_blk
    qc, oc = q_width // n_q, hidden // n_o
    rep = q_heads // kv_heads

    def copy_q(i):
        cols = pl.ds(pl.multiple_of(i * qc, qc), qc)
        return pltpu.make_async_copy(wq_hbm.at[:, cols], wq.at[:, cols], s_q.at[i])

    def copy_o(i):
        cols = pl.ds(pl.multiple_of(i * oc, oc), oc)
        return pltpu.make_async_copy(wo_hbm.at[:, cols], wo.at[:, cols], s_o.at[i])

    def copy_in(b):
        rows = pl.ds(b * blk, blk)
        return (pltpu.make_async_copy(kc_hbm.at[rows], kbuf.at[rows], s_c.at[0, b]),
                pltpu.make_async_copy(vc_hbm.at[rows], vbuf.at[rows], s_c.at[1, b]))

    def copy_out(b):
        rows = pl.ds(b * blk, blk)
        return (pltpu.make_async_copy(kbuf.at[rows], ko_hbm.at[rows], s_out.at[0, b]),
                pltpu.make_async_copy(vbuf.at[rows], vo_hbm.at[rows], s_out.at[1, b]))

    small = (pltpu.make_async_copy(wk_hbm, wk, s_kv.at[0]), pltpu.make_async_copy(wv_hbm, wv, s_kv.at[1]),
             pltpu.make_async_copy(wr_hbm, wr, s_kv.at[2]))
    for c in small[:2]:
        c.start()
    for i in range(n_q):
        copy_q(i).start()
    for b in range(n_blk):
        for c in copy_in(b):
            c.start()
    for i in range(n_o):
        copy_o(i).start()
    small[2].start()

    x = x_ref[...].astype(F32)
    hn[...] = rms(x, lna_ref[...].astype(F32)).astype(BF16)
    cos, sin = cos_ref[...], sin_ref[...]

    def turned(values, gain):
        normed = rms(values, gain)
        return (normed * cos + pltpu.roll(normed, dim // 2, 1) * sin).astype(BF16).astype(F32)

    small[0].wait()
    small[1].wait()
    key = jnp.dot(hn[...], wk[...], preferred_element_type=F32)
    val = jnp.dot(hn[...], wv[...], preferred_element_type=F32).astype(BF16).astype(F32)
    for g in range(kv_heads):
        cols = slice(g * dim, (g + 1) * dim)
        turned_k = turned(key[:, cols], kn_ref[...].astype(F32))
        for r in range(8 // kv_heads):
            rows = pl.ds(g + kv_heads * r, b_dev, stride=8)
            knew[rows, :] = turned_k
            vnew[rows, :] = val[:, cols]
    for i in range(n_q):
        copy_q(i).wait()
        part = jnp.dot(hn[...], wq[:, i * qc:(i + 1) * qc], preferred_element_type=F32)
        for j in range(qc // dim):
            qs[pl.ds(i * (qc // dim) + j, b_dev, stride=q_heads), :] = turned(
                part[:, j * dim:(j + 1) * dim], qn_ref[...].astype(F32))

    row_slot = lax.broadcasted_iota(jnp.int32, (lanes, dim), 0) // kv_heads
    lane = lax.broadcasted_iota(jnp.int32, (q_heads, lanes), 1)
    own_head = lax.rem(lane, kv_heads) == lax.broadcasted_iota(jnp.int32, (q_heads, lanes), 0) // rep
    lane_slot = jnp.where(own_head, lane // kv_heads, lanes)

    @pl.loop(0, n_blk)
    def _(b):
        for c in copy_in(b):
            c.wait()
        scores = []
        for j in range(blk):
            t = b * blk + j
            size = len_ref[t]
            here = row_slot == size
            fresh = pl.ds(pl.multiple_of(t * 8, 8), 8)
            k_row = jnp.concatenate([knew[fresh, :]] * (lanes // 8), axis=0)
            v_row = jnp.concatenate([vnew[fresh, :]] * (lanes // 8), axis=0)
            k_tok = jnp.where(here, k_row, kbuf[t].astype(F32)).astype(BF16)
            kbuf[t] = k_tok
            vbuf[t] = jnp.where(here, v_row, vbuf[t].astype(F32)).astype(BF16)
            q_tok = qs[pl.ds(pl.multiple_of(t * q_heads, q_heads), q_heads), :].astype(BF16)
            score = lax.dot_general(q_tok, k_tok, (((1,), (1,)), ((), ())), preferred_element_type=F32)
            scores.append(jnp.where(lane_slot <= size, score * dim ** -0.5, -1e30))
        score = jnp.concatenate(scores, axis=0)
        weight = jnp.exp(score - jnp.max(score, axis=1, keepdims=True))
        prob = (weight / jnp.sum(weight, axis=1, keepdims=True)).astype(BF16)
        for j in range(blk):
            t = b * blk + j
            os[pl.ds(pl.multiple_of(t * q_heads, q_heads), q_heads), :] = jnp.dot(
                prob[j * q_heads:(j + 1) * q_heads, :], vbuf[t], preferred_element_type=F32)
        for c in copy_out(b):
            c.start()

    for h in range(q_heads):
        att[:, h * dim:(h + 1) * dim] = os[pl.ds(h, b_dev, stride=q_heads), :].astype(BF16)
    for i in range(n_o):
        copy_o(i).wait()
        cols = slice(i * oc, (i + 1) * oc)
        out = jnp.dot(att[...], wo[:, cols], preferred_element_type=F32)
        xmid_ref[:, cols] = (x_ref[:, cols].astype(F32) + out).astype(BF16)
    h_moe = rms(xmid_ref[...].astype(F32), lnm_ref[...].astype(F32)).astype(BF16)
    h_ref[...] = h_moe
    small[2].wait()
    logits = jnp.transpose(jnp.dot(h_moe, wr[...], preferred_element_type=F32))
    experts = logits.shape[0]
    e_local = experts // ep_size
    expert = lax.broadcasted_iota(jnp.int32, (experts, b_dev), 0)
    chosen = expert == idx_ref[0:1, :]
    for k in range(1, idx_ref.shape[0]):
        chosen = chosen | (expert == idx_ref[k:k + 1, :])
    top = jnp.max(jnp.where(chosen, logits, -1e30), axis=0, keepdims=True)
    mass = jnp.where(chosen, jnp.exp(logits - top), 0.0)
    mass = mass / jnp.sum(mass, axis=0, keepdims=True)
    local = jnp.where(chosen, lax.rem(expert, e_local), 0).astype(F32)
    meta_ref[0:ep_size, :] = jnp.sum(local.reshape(ep_size, e_local, b_dev), axis=1)
    meta_ref[ep_size:2 * ep_size, :] = jnp.sum(mass.reshape(ep_size, e_local, b_dev), axis=1)

    for b in range(n_blk):
        for c in copy_out(b):
            c.wait()


def attend_block(ep_size, x_in, k_cache, v_cache, cache_len, topk_idx, ln_attn, w_q, w_k, w_v, q_norm, k_norm, w_o, ln_moe, w_router):
    b_dev, hidden = x_in.shape
    _, n_slots, kv_heads, dim = k_cache.shape
    q_width, kv_width, experts = w_q.shape[1], w_k.shape[1], w_router.shape[1]
    q_heads = q_width // dim
    lanes = n_slots * kv_heads
    freq = ROPE_BASE ** (-jnp.arange(dim // 2, dtype=F32) * 2.0 / dim)
    angles = cache_len.astype(F32)[:, None] * freq
    cosine, sine = jnp.cos(angles), jnp.sin(angles)
    cos = jnp.concatenate([cosine, cosine], axis=1)
    sin = jnp.concatenate([-sine, sine], axis=1)
    n_q, n_o, n_blk = 8, 4, 8
    vmem, dma, far = pltpu.VMEM, pltpu.SemaphoreType.DMA, pl.BlockSpec(memory_space=pl.ANY)
    near = pl.BlockSpec(memory_space=pltpu.VMEM)
    flat = (b_dev, lanes, dim)
    x_mid, h_moe, meta, k_new, v_new = pl.pallas_call(
        functools.partial(attend_kernel, ep_size),
        out_shape=(jax.ShapeDtypeStruct((b_dev, hidden), BF16), jax.ShapeDtypeStruct((b_dev, hidden), BF16),
                   jax.ShapeDtypeStruct((2 * ep_size, b_dev), F32),
                   jax.ShapeDtypeStruct(flat, BF16), jax.ShapeDtypeStruct(flat, BF16)),
        in_specs=[pl.BlockSpec(memory_space=pltpu.SMEM)] + [near] * 8 + [far] * 7,
        out_specs=(near, near, near, far, far),
        scratch_shapes=[
            vmem((hidden, q_width), BF16), vmem((hidden, kv_width), BF16), vmem((hidden, kv_width), BF16),
            vmem((q_width, hidden), BF16), vmem((hidden, experts), BF16), vmem(flat, BF16), vmem(flat, BF16),
            vmem((b_dev * q_heads, dim), F32), vmem((b_dev * q_heads, dim), F32),
            vmem((b_dev * 8, dim), F32), vmem((b_dev * 8, dim), F32),
            vmem((b_dev, hidden), BF16), vmem((b_dev, q_width), BF16),
            dma((n_q,)), dma((3,)), dma((n_o,)), dma((2, n_blk)), dma((2, n_blk)),
        ],
        compiler_params=pltpu.CompilerParams(vmem_limit_bytes=67043328),
        name='attend',
    )(cache_len, x_in, cos, sin, topk_idx.T, ln_attn[None], q_norm[None], k_norm[None], ln_moe[None],
      w_q, w_k, w_v, w_o, w_router, k_cache.reshape(flat), v_cache.reshape(flat))
    return x_mid, h_moe, meta, k_new.reshape(k_cache.shape), v_new.reshape(v_cache.shape)


def moe_kernel(ep_size, h_ref, x_ref, meta_ref, wg_hbm, wu_hbm, wd_hbm, out_ref, flag_ref,
               xall, mall, perm, keys, keyt, xg, hid, ys, ybuf, yrecv, zsum, recv1, recv2, fin,
               wg, wu, wd, s_w, s_d, s_own, s_fwd, s_pair, r_x, s_meta, r_meta,
               s_y, r_y, s_1, r_1, s_2, r_2, s_f, r_f):
    b_dev, hidden = h_ref.shape
    e_local, _, ff = wg_hbm.shape
    n_chip = ep_size // 2
    half = b_dev // 2
    wide = hidden // SPLIT
    side = wide // 2
    n_a, n_b = wg.shape[0], wd.shape[0]
    per = wd.shape[1]
    groups = e_local // per
    me = lax.axis_index('ep')
    chip, core = me // 2, me % 2
    right = lax.rem(chip + 1, n_chip)
    left = lax.rem(chip + n_chip - 1, n_chip)
    far = lax.rem(chip + 2, n_chip)
    dev_r, dev_l, mate = right * 2 + core, left * 2 + core, chip * 2 + 1 - core

    def load_a(e):
        slot = lax.rem(e, n_a)
        return (pltpu.make_async_copy(wg_hbm.at[e], wg.at[slot], s_w.at[0, slot]),
                pltpu.make_async_copy(wu_hbm.at[e], wu.at[slot], s_w.at[1, slot]))

    def load_b(i):
        slot = lax.rem(i, n_b)
        q, g = i // groups, lax.rem(i, groups)
        cols = pl.ds(pl.multiple_of(q * wide, wide), wide)
        return pltpu.make_async_copy(wd_hbm.at[pl.ds(g * per, per), :, cols], wd.at[slot], s_d.at[slot])

    for e in range(n_a):
        for c in load_a(e):
            c.start()
    for i in range(n_b):
        load_b(i).start()

    barrier = pltpu.get_barrier_semaphore()
    for k in range(1, ep_size):
        pl.semaphore_signal(barrier, inc=1, device_id={'ep': lax.rem(me + k, ep_size)}, device_id_type=MESH)
    pl.semaphore_wait(barrier, ep_size - 1)

    def part(h):
        return pl.ds(h * half, half)

    def send_own(h, target, sem):
        return pltpu.make_async_remote_copy(h_ref.at[part(h)], xall.at[me, part(h)], sem, r_x.at[me, h],
                                            device_id={'ep': target}, device_id_type=MESH)

    def forward(src, h, target, sem):
        return pltpu.make_async_remote_copy(xall.at[src, part(h)], xall.at[src, part(h)], sem, r_x.at[src, h],
                                            device_id={'ep': target}, device_id_type=MESH)

    def send_meta(k):
        return pltpu.make_async_remote_copy(meta_ref, mall.at[me], s_meta.at[k - 1], r_meta.at[me],
                                            device_id={'ep': lax.rem(me + k, ep_size)}, device_id_type=MESH)

    started = []

    def go(copy):
        copy.start()
        started.append(copy)

    for k in range(1, ep_size):
        go(send_meta(k))
    go(send_own(0, dev_r, s_own.at[0]))
    go(send_own(1, dev_l, s_own.at[1]))
    go(send_own(1, dev_r, s_own.at[2]))
    go(send_own(0, dev_l, s_own.at[3]))
    go(send_own(0, mate, s_own.at[4]))
    go(send_own(1, mate, s_own.at[5]))
    xall[me] = h_ref[...]
    mall[me] = meta_ref[...]

    forward(dev_l, 0, dev_r, s_fwd.at[0]).wait_recv()
    go(forward(dev_l, 0, dev_r, s_fwd.at[0]))
    go(forward(dev_l, 0, mate, s_pair.at[0]))
    forward(dev_r, 1, dev_l, s_fwd.at[1]).wait_recv()
    go(forward(dev_r, 1, dev_l, s_fwd.at[1]))
    go(forward(dev_r, 1, mate, s_pair.at[1]))

    for k in range(1, ep_size):
        src = lax.rem(me + k, ep_size)
        pltpu.make_async_remote_copy(meta_ref, mall.at[src], s_meta.at[k - 1], r_meta.at[src],
                                     device_id={'ep': src}, device_id_type=MESH).wait_recv()
    lower = lax.broadcasted_iota(jnp.int32, (b_dev, b_dev), 0) < lax.broadcasted_iota(jnp.int32, (b_dev, b_dev), 1)
    before = jnp.where(lower, 1.0, 0.0).astype(BF16)
    ids16 = lax.broadcasted_iota(jnp.int32, (e_local, b_dev), 0).astype(F32)
    keys[...] = jnp.zeros_like(keys)
    counts = jnp.zeros((e_local, 1), F32)
    for src in range(ep_size):
        row = mall[src, pl.ds(me, 1), :]
        hot = jnp.where(ids16 == row, 1.0, 0.0)
        ranks = jnp.dot(hot.astype(BF16), before, preferred_element_type=F32) + counts
        rank = jnp.sum(hot * ranks, axis=0, keepdims=True)
        keys[pl.ds(src, 1), :] = row * SEATS + rank
        keys[pl.ds(ep_size + src, 1), :] = mall[src, pl.ds(ep_size + me, 1), :]
        keys[pl.ds(2 * ep_size + src, 1), :] = mall[src, pl.ds(ep_size + mate, 1), :]
        counts = counts + jnp.sum(hot, axis=1, keepdims=True)
    keyt[...] = jnp.transpose(keys[...])
    most = jnp.zeros((e_local, 1), F32)
    for dev in range(ep_size):
        total = jnp.zeros((e_local, 1), F32)
        for src in range(ep_size):
            hot = jnp.where(ids16 == mall[src, pl.ds(dev, 1), :], 1.0, 0.0)
            total = total + jnp.sum(hot, axis=1, keepdims=True)
        most = jnp.maximum(most, total)
    flag_ref[...] = jnp.broadcast_to(jnp.max(most, axis=0, keepdims=True), flag_ref.shape)

    seat_cols = lax.broadcasted_iota(jnp.int32, (b_dev, 4 * SEATS), 1).astype(F32)
    for b in range(ep_size):
        col = keyt[:, b:b + 1]

        @pl.loop(0, e_local // 4)
        def _(j):
            base = (j * (4 * SEATS)).astype(F32)
            hot = jnp.where(seat_cols + base == col, 1.0, 0.0).astype(BF16)
            perm[b * b_dev:(b + 1) * b_dev, pl.ds(pl.multiple_of(j * (4 * SEATS), 4 * SEATS), 4 * SEATS)] = hot

    for src, h, sem in ((dev_l, 1, 2), (dev_r, 0, 3)):
        forward(src, h, mate, s_pair.at[sem]).wait_recv()
        go(forward(src, h, mate, s_pair.at[sem]))
    dev_f = far * 2 + core
    for h in range(2):
        forward(dev_f, h, mate, s_pair.at[4 + h]).wait_recv()
        go(forward(dev_f, h, mate, s_pair.at[4 + h]))
    for k in range(n_chip):
        src = lax.rem(chip + k, n_chip) * 2 + 1 - core
        for h in range(2):
            forward(src, h, mate, s_pair.at[h]).wait_recv()

    seat_rows = lax.broadcasted_iota(jnp.int32, (SEATS, b_dev), 0).astype(F32)

    @pl.loop(0, e_local)
    def _(e):
        slot = lax.rem(e, n_a)
        base = (e * SEATS).astype(F32)
        pick = jnp.concatenate(
            [jnp.where(keys[b:b + 1, :] == seat_rows + base, 1.0, 0.0).astype(BF16) for b in range(ep_size)], axis=1)
        for n in range(4):
            cols = slice(n * (hidden // 4), (n + 1) * (hidden // 4))
            rows = xall[:, :, cols].reshape(ep_size * b_dev, hidden // 4)
            xg[:, cols] = jnp.dot(pick, rows, preferred_element_type=F32).astype(BF16)
        for c in load_a(e):
            c.wait()
        for n in range(ff // 256):
            cols = slice(n * 256, (n + 1) * 256)
            gate = jnp.dot(xg[...], wg[slot, :, cols], preferred_element_type=F32)
            up = jnp.dot(xg[...], wu[slot, :, cols], preferred_element_type=F32)
            hid[e, :, cols] = (gate * jax.nn.sigmoid(gate) * up).astype(BF16)

        @pl.when(e + n_a < e_local)
        def _():
            for c in load_a(e + n_a):
                c.start()

    def send_y(q):
        return pltpu.make_async_remote_copy(ybuf.at[q, 1 - core], yrecv.at[q], s_y.at[q], r_y.at[q],
                                            device_id={'ep': mate}, device_id_type=MESH)

    def send_1(q, d):
        block = far * 2 + d
        return pltpu.make_async_remote_copy(zsum.at[q, block], recv1.at[d, q], s_1.at[d, q], r_1.at[d, q],
                                            device_id={'ep': dev_l if d else dev_r}, device_id_type=MESH)

    def send_2(q, d):
        block = (left if d else right) * 2
        return pltpu.make_async_remote_copy(zsum.at[q, pl.ds(block, 2)], recv2.at[d, q], s_2.at[d, q], r_2.at[d, q],
                                            device_id={'ep': dev_l if d else dev_r}, device_id_type=MESH)

    def send_f(q):
        return pltpu.make_async_remote_copy(zsum.at[q, mate], fin.at[q], s_f.at[q], r_f.at[q],
                                            device_id={'ep': mate}, device_id_type=MESH)

    def relay(q):
        for d in range(2):
            send_1(q, d).wait_recv()
            block = (left if d else right) * 2 + d
            zsum[q, block] = zsum[q, block] + recv1[d, q]
            send_2(q, d).start()

    @pl.loop(0, SPLIT)
    def _(q):
        @pl.loop(0, groups)
        def _(g):
            i = q * groups + g
            slot = lax.rem(i, n_b)
            load_b(i).wait()
            for j in range(per):
                e = g * per + j
                ys[pl.ds(pl.multiple_of(e * SEATS, SEATS), SEATS), :] = jnp.dot(
                    hid[e], wd[slot, j], preferred_element_type=F32).astype(BF16)

            @pl.when(i + n_b < SPLIT * groups)
            def _():
                load_b(i + n_b).start()

        @pl.loop(0, ep_size // 2)
        def _(m):
            rows = pl.ds(pl.multiple_of(m * (2 * b_dev), 2 * b_dev), 2 * b_dev)
            for h in range(2):
                part_y = jnp.dot(perm[rows, :], ys[:, h * side:(h + 1) * side], preferred_element_type=F32)
                ybuf[q, h, pl.ds(2 * m, 2)] = part_y.astype(BF16).reshape(2, b_dev, side)

        send_y(q).start()

        @pl.when(q > 0)
        def _():
            relay(q - 1)

        send_y(q).wait_recv()
        for b in range(ep_size):
            zsum[q, b] = (keyt[:, ep_size + b:ep_size + b + 1] * ybuf[q, core, b].astype(F32)
                          + keyt[:, 2 * ep_size + b:2 * ep_size + b + 1] * yrecv[q, b].astype(F32))
        send_1(q, 0).start()
        send_1(q, 1).start()

    relay(SPLIT - 1)

    def columns(q, which):
        return pl.ds(pl.multiple_of(q * wide + which * side, side), side)

    @pl.loop(0, SPLIT)
    def _(q):
        send_2(q, 0).wait_recv()
        send_2(q, 1).wait_recv()
        zsum[q, mate] = zsum[q, mate] + recv2[0, q, 1 - core] + recv2[1, q, 1 - core]
        send_f(q).start()
        mine = zsum[q, me] + recv2[0, q, core] + recv2[1, q, core]
        cols = columns(q, core)
        out_ref[:, cols] = (x_ref[:, cols].astype(F32) + mine).astype(BF16)

    @pl.loop(0, SPLIT)
    def _(q):
        send_f(q).wait_recv()
        cols = columns(q, 1 - core)
        out_ref[:, cols] = (x_ref[:, cols].astype(F32) + fin[q]).astype(BF16)

    for copy in started:
        copy.wait_send()

    @pl.loop(0, SPLIT)
    def _(q):
        send_y(q).wait_send()
        send_f(q).wait_send()
        for d in range(2):
            send_1(q, d).wait_send()
            send_2(q, d).wait_send()


def moe_block(ep_size, h_moe, x_mid, meta, w_gate, w_up, w_down):
    b_dev, hidden = h_moe.shape
    e_local, _, ff = w_gate.shape
    wide, side = hidden // SPLIT, hidden // SPLIT // 2
    n_a, n_b, per = 3, 4, 4
    vmem, dma = pltpu.VMEM, pltpu.SemaphoreType.DMA
    tokens = ep_size * b_dev
    return pl.pallas_call(
        functools.partial(moe_kernel, ep_size),
        out_shape=(jax.ShapeDtypeStruct((b_dev, hidden), BF16), jax.ShapeDtypeStruct((8, 128), F32)),
        in_specs=[pl.BlockSpec(memory_space=pltpu.VMEM)] * 3 + [pl.BlockSpec(memory_space=pl.ANY)] * 3,
        out_specs=(pl.BlockSpec(memory_space=pltpu.VMEM), pl.BlockSpec(memory_space=pltpu.VMEM)),
        scratch_shapes=[
            vmem((ep_size, b_dev, hidden), BF16), vmem((ep_size, 2 * ep_size, b_dev), F32),
            vmem((tokens, e_local * SEATS), BF16), vmem((b_dev, b_dev), F32), vmem((b_dev, b_dev), F32),
            vmem((SEATS, hidden), BF16), vmem((e_local, SEATS, ff), BF16), vmem((e_local * SEATS, wide), BF16),
            vmem((SPLIT, 2, ep_size, b_dev, side), BF16), vmem((SPLIT, ep_size, b_dev, side), BF16),
            vmem((SPLIT, ep_size, b_dev, side), F32), vmem((2, SPLIT, b_dev, side), F32),
            vmem((2, SPLIT, 2, b_dev, side), F32), vmem((SPLIT, b_dev, side), F32),
            vmem((n_a, hidden, ff), BF16), vmem((n_a, hidden, ff), BF16), vmem((n_b, per, ff, wide), BF16),
            dma((2, n_a)), dma((n_b,)), dma((6,)), dma((2,)), dma((6,)), dma((ep_size, 2)),
            dma((ep_size - 1,)), dma((ep_size,)),
            dma((SPLIT,)), dma((SPLIT,)), dma((2, SPLIT)), dma((2, SPLIT)), dma((2, SPLIT)), dma((2, SPLIT)),
            dma((SPLIT,)), dma((SPLIT,)),
        ],
        compiler_params=pltpu.CompilerParams(collective_id=0, has_side_effects=True, vmem_limit_bytes=67043328),
        name='moe',
    )(h_moe, x_mid, meta, w_gate, w_up, w_down)


def moe_general(ep_size, h_moe, x_mid, meta, w_gate, w_up, w_down):
    b_dev, hidden = h_moe.shape
    rows = lax.all_to_all(jnp.broadcast_to(h_moe[None], (ep_size, b_dev, hidden)), 'ep', 0, 0, tiled=True)
    rows = rows.reshape(ep_size * b_dev, hidden)
    ids = lax.all_to_all(meta[:ep_size, None, :], 'ep', 0, 0, tiled=True).reshape(ep_size * b_dev)

    def one(e, done):
        gate = jnp.dot(rows, w_gate[e], preferred_element_type=F32)
        up = jnp.dot(rows, w_up[e], preferred_element_type=F32)
        act = (jax.nn.silu(gate) * up).astype(BF16)
        y = jnp.dot(act, w_down[e], preferred_element_type=F32).astype(BF16)
        return jnp.where((ids == e.astype(F32))[:, None], y, done)

    y = lax.fori_loop(0, w_gate.shape[0], one, jnp.zeros(rows.shape, BF16))
    back = lax.all_to_all(y.reshape(ep_size, b_dev, hidden), 'ep', 0, 0, tiled=True)
    total = jnp.sum(back.astype(F32) * meta[ep_size:, :, None], axis=0)
    return (x_mid.astype(F32) + total).astype(BF16)


def solution(mesh):
    ep_size = mesh.shape['ep']
    row_spec = P(('dp', 'ep'))
    replicated = P()
    expert_spec = P('ep')
    in_specs = (row_spec,) * 5 + (replicated,) * 9 + (expert_spec,) * 3
    out_specs = (row_spec, row_spec, row_spec)

    def device_step(x_in, k_cache, v_cache, cache_len, topk_idx, ln_attn, w_q, w_k, w_v, q_norm, k_norm, w_o, ln_moe, w_router, w_gate, w_up, w_down):
        x_mid, h_moe, meta, k_full, v_full = attend_block(
            ep_size, x_in, k_cache, v_cache, cache_len, topk_idx, ln_attn, w_q, w_k, w_v, q_norm, k_norm, w_o, ln_moe, w_router)
        fast, most = moe_block(ep_size, h_moe, x_mid, meta, w_gate, w_up, w_down)
        x_out = lax.cond(most[0, 0] > SEATS,
                         lambda: moe_general(ep_size, h_moe, x_mid, meta, w_gate, w_up, w_down),
                         lambda: fast)
        return x_out, k_full, v_full

    return jax.shard_map(device_step, mesh=mesh, in_specs=in_specs, out_specs=out_specs, check_vma=False)
```

```python
import functools
import math

import jax
import jax.numpy as jnp
from jax import lax
from jax.experimental import pallas as pl
from jax.experimental.pallas import tpu as pltpu
from jax.sharding import PartitionSpec as P

ROPE_BASE = 1000000.0
NORM_EPS = 1e-6
MESH = pl.DeviceIdType.MESH
F32 = jnp.float32
BF16 = jnp.bfloat16
SEATS = 128
SPLIT = 4
DEEP = 2


def rms(values):
    return values * lax.rsqrt(jnp.mean(values * values, axis=-1, keepdims=True) + NORM_EPS)


def rms_rows(values, gain_ref, out_ref):
    normed = rms(values)
    lanes = gain_ref.shape[1]
    for i in range(gain_ref.shape[0]):
        cols = slice(i * lanes, (i + 1) * lanes)
        out_ref[:, cols] = (normed[:, cols] * gain_ref[i:i + 1, :].astype(F32)).astype(BF16)


def attend_kernel(ep_size, len_ref, x_ref, row_ref, idx_ref, lna_ref, qn_ref, kn_ref, lnm_ref,
                  wq_hbm, wk_hbm, wv_hbm, wo_hbm, wr_hbm, kc_hbm, vc_hbm,
                  xmid_ref, h_ref, meta_ref, ko_hbm, vo_hbm,
                  wq, wk, wv, wo, wr, kbuf, vbuf, qs, os, knew, vnew, hn, att, part,
                  s_q, s_kv, s_o, s_c, s_out):
    b_dev, hidden = x_ref.shape
    _, lanes, dim = kbuf.shape
    q_width = wq.shape[1]
    q_heads, kv_heads = q_width // dim, wk.shape[1] // dim
    n_q, n_o = s_q.shape[0], s_o.shape[0]
    n_blk = s_c.shape[1]
    blk = b_dev // n_blk
    qc, oc = q_width // n_q, hidden // n_o
    rep = q_heads // kv_heads

    def copy_q(i):
        cols = pl.ds(pl.multiple_of(i * qc, qc), qc)
        return pltpu.make_async_copy(wq_hbm.at[:, cols], wq.at[:, cols], s_q.at[i])

    def copy_o(i):
        cols = pl.ds(pl.multiple_of(i * oc, oc), oc)
        return pltpu.make_async_copy(wo_hbm.at[:, cols], wo.at[:, cols], s_o.at[i])

    def copy_in(b):
        rows = pl.ds(b * blk, blk)
        return (pltpu.make_async_copy(kc_hbm.at[rows], kbuf.at[rows], s_c.at[0, b]),
                pltpu.make_async_copy(vc_hbm.at[rows], vbuf.at[rows], s_c.at[1, b]))

    def copy_out(b):
        rows = pl.ds(b * blk, blk)
        return (pltpu.make_async_copy(kbuf.at[rows], ko_hbm.at[rows], s_out.at[0, b]),
                pltpu.make_async_copy(vbuf.at[rows], vo_hbm.at[rows], s_out.at[1, b]))

    small = (pltpu.make_async_copy(wk_hbm, wk, s_kv.at[0]), pltpu.make_async_copy(wv_hbm, wv, s_kv.at[1]),
             pltpu.make_async_copy(wr_hbm, wr, s_kv.at[2]))
    for c in small[:2]:
        c.start()
    for i in range(n_q):
        copy_q(i).start()

    x = x_ref[...].astype(F32)
    rms_rows(x, lna_ref, hn)
    pair = lax.rem(lax.broadcasted_iota(jnp.int32, (b_dev, dim), 1), dim // 2).astype(F32)
    freq = jnp.exp(pair * (-2.0 / dim * math.log(ROPE_BASE)))
    angle = jnp.transpose(jnp.broadcast_to(row_ref[...].astype(F32), (dim, b_dev))) * freq
    cos = jnp.cos(angle)
    sin = jnp.where(lax.broadcasted_iota(jnp.int32, (b_dev, dim), 1) < dim // 2, -1.0, 1.0) * jnp.sin(angle)

    def turned(values, gain):
        normed = rms(values) * gain
        return (normed * cos + pltpu.roll(normed, dim // 2, 1) * sin).astype(BF16).astype(F32)

    small[0].wait()
    small[1].wait()
    key = jnp.dot(hn[...], wk[...], preferred_element_type=F32)
    val = jnp.dot(hn[...], wv[...], preferred_element_type=F32).astype(BF16).astype(F32)
    for g in range(kv_heads):
        cols = slice(g * dim, (g + 1) * dim)
        turned_k = turned(key[:, cols], kn_ref[...].astype(F32))
        for r in range(8 // kv_heads):
            rows = pl.ds(g + kv_heads * r, b_dev, stride=8)
            knew[rows, :] = turned_k
            vnew[rows, :] = val[:, cols]
    def spread(i):
        for j in range(qc // dim):
            qs[pl.ds(i * (qc // dim) + j, b_dev, stride=q_heads), :] = turned(
                part[i % 2, :, j * dim:(j + 1) * dim], qn_ref[...].astype(F32))

    for i in range(n_q):
        copy_q(i).wait()
        if i == 1:
            for b in range(n_blk):
                for c in copy_in(b):
                    c.start()
        if i == 4:
            for j in range(n_o):
                copy_o(j).start()
            small[2].start()
        part[i % 2] = jnp.dot(hn[...], wq[:, i * qc:(i + 1) * qc], preferred_element_type=F32)
        if i:
            spread(i - 1)
    spread(n_q - 1)

    row_slot = lax.broadcasted_iota(jnp.int32, (lanes, dim), 0) // kv_heads
    lane = lax.broadcasted_iota(jnp.int32, (q_heads, lanes), 1)
    own_head = lax.rem(lane, kv_heads) == lax.broadcasted_iota(jnp.int32, (q_heads, lanes), 0) // rep
    lane_slot = jnp.where(own_head, lane // kv_heads, lanes)

    @pl.loop(0, n_blk)
    def _(b):
        for c in copy_in(b):
            c.wait()
        scores = []
        for j in range(blk):
            t = b * blk + j
            size = len_ref[t]
            here = row_slot == size
            fresh = pl.ds(pl.multiple_of(t * 8, 8), 8)
            k_row = jnp.concatenate([knew[fresh, :]] * (lanes // 8), axis=0)
            v_row = jnp.concatenate([vnew[fresh, :]] * (lanes // 8), axis=0)
            k_tok = jnp.where(here, k_row, kbuf[t].astype(F32)).astype(BF16)
            kbuf[t] = k_tok
            vbuf[t] = jnp.where(here, v_row, vbuf[t].astype(F32)).astype(BF16)
            q_tok = qs[pl.ds(pl.multiple_of(t * q_heads, q_heads), q_heads), :].astype(BF16)
            score = lax.dot_general(q_tok, k_tok, (((1,), (1,)), ((), ())), preferred_element_type=F32)
            scores.append(jnp.where(lane_slot <= size, score * dim ** -0.5, -1e30))
        score = jnp.concatenate(scores, axis=0)
        weight = jnp.exp(score - jnp.max(score, axis=1, keepdims=True))
        prob = (weight / jnp.sum(weight, axis=1, keepdims=True)).astype(BF16)
        for j in range(blk):
            t = b * blk + j
            os[pl.ds(pl.multiple_of(t * q_heads, q_heads), q_heads), :] = jnp.dot(
                prob[j * q_heads:(j + 1) * q_heads, :], vbuf[t], preferred_element_type=F32)
        for c in copy_out(b):
            c.start()

    for h in range(q_heads):
        att[:, h * dim:(h + 1) * dim] = os[pl.ds(h, b_dev, stride=q_heads), :].astype(BF16)
    for i in range(n_o):
        copy_o(i).wait()
        cols = slice(i * oc, (i + 1) * oc)
        out = jnp.dot(att[...], wo[:, cols], preferred_element_type=F32)
        xmid_ref[:, cols] = (x_ref[:, cols].astype(F32) + out).astype(BF16)
    rms_rows(xmid_ref[...].astype(F32), lnm_ref, h_ref)
    small[2].wait()
    logits = jnp.transpose(jnp.dot(h_ref[...], wr[...], preferred_element_type=F32))
    experts = logits.shape[0]
    e_local = experts // ep_size
    expert = lax.broadcasted_iota(jnp.int32, (experts, b_dev), 0)
    chosen = expert == idx_ref[0:1, :]
    for k in range(1, idx_ref.shape[0]):
        chosen = chosen | (expert == idx_ref[k:k + 1, :])
    top = jnp.max(jnp.where(chosen, logits, -1e30), axis=0, keepdims=True)
    mass = jnp.where(chosen, jnp.exp(logits - top), 0.0)
    mass = mass / jnp.sum(mass, axis=0, keepdims=True)
    local = jnp.where(chosen, lax.rem(expert, e_local), 0).astype(F32)
    meta_ref[0:ep_size, :] = jnp.sum(local.reshape(ep_size, e_local, b_dev), axis=1)
    meta_ref[ep_size:2 * ep_size, :] = jnp.sum(mass.reshape(ep_size, e_local, b_dev), axis=1)

    for b in range(n_blk):
        for c in copy_out(b):
            c.wait()


def attend_block(ep_size, x_in, k_cache, v_cache, cache_len, topk_idx, ln_attn, w_q, w_k, w_v, q_norm, k_norm, w_o, ln_moe, w_router):
    b_dev, hidden = x_in.shape
    _, n_slots, kv_heads, dim = k_cache.shape
    q_width, kv_width, experts = w_q.shape[1], w_k.shape[1], w_router.shape[1]
    q_heads = q_width // dim
    lanes = n_slots * kv_heads
    n_q, n_o, n_blk = 8, 4, 8
    vmem, dma, far = pltpu.VMEM, pltpu.SemaphoreType.DMA, pl.BlockSpec(memory_space=pl.ANY)
    near = pl.BlockSpec(memory_space=pltpu.VMEM)
    flat = (b_dev, lanes, dim)
    x_mid, h_moe, meta, k_new, v_new = pl.pallas_call(
        functools.partial(attend_kernel, ep_size),
        out_shape=(jax.ShapeDtypeStruct((b_dev, hidden), BF16), jax.ShapeDtypeStruct((b_dev, hidden), BF16),
                   jax.ShapeDtypeStruct((2 * ep_size, b_dev), F32),
                   jax.ShapeDtypeStruct(flat, BF16), jax.ShapeDtypeStruct(flat, BF16)),
        in_specs=[pl.BlockSpec(memory_space=pltpu.SMEM)] + [near] * 7 + [far] * 7,
        out_specs=(near, near, near, far, far),
        scratch_shapes=[
            vmem((hidden, q_width), BF16), vmem((hidden, kv_width), BF16), vmem((hidden, kv_width), BF16),
            vmem((q_width, hidden), BF16), vmem((hidden, experts), BF16), vmem(flat, BF16), vmem(flat, BF16),
            vmem((b_dev * q_heads, dim), F32), vmem((b_dev * q_heads, dim), F32),
            vmem((b_dev * 8, dim), F32), vmem((b_dev * 8, dim), F32),
            vmem((b_dev, hidden), BF16), vmem((b_dev, q_width), BF16), vmem((2, b_dev, q_width // n_q), F32),
            dma((n_q,)), dma((3,)), dma((n_o,)), dma((2, n_blk)), dma((2, n_blk)),
        ],
        compiler_params=pltpu.CompilerParams(vmem_limit_bytes=67043328),
        name='attend',
    )(cache_len, x_in, cache_len[None], topk_idx.T, ln_attn.reshape(-1, dim), q_norm[None], k_norm[None], ln_moe.reshape(-1, dim),
      w_q, w_k, w_v, w_o, w_router, k_cache.reshape(flat), v_cache.reshape(flat))
    return x_mid, h_moe, meta, k_new.reshape(k_cache.shape), v_new.reshape(v_cache.shape)


def moe_kernel(ep_size, h_ref, x_ref, meta_ref, wg_hbm, wu_hbm, wd_hbm, out_ref, flag_ref,
               xall, mall, perm, keys, share, xg_even, xg_odd, hid, ys, ybuf, yrecv, acc, recv1, recv2, fin,
               wg, wu, wd, s_w, s_d, s_own, s_fwd, r_x, s_meta, r_meta,
               s_y, r_y, s_1, r_1, s_2, r_2, s_f, r_f):
    b_dev, hidden = h_ref.shape
    e_local, _, ff = wg_hbm.shape
    n_chip = ep_size // 2
    half = b_dev // 2
    depth = hidden // DEEP
    wide = hidden // SPLIT
    side = wide // 2
    n_a, n_b = wg.shape[0], wd.shape[0]
    per = wd.shape[1]
    groups = e_local // per
    me = lax.axis_index('ep')
    chip, core = me // 2, me % 2
    right = lax.rem(chip + 1, n_chip)
    left = lax.rem(chip + n_chip - 1, n_chip)
    far = lax.rem(chip + 2, n_chip)
    dev_r, dev_l, mate = right * 2 + core, left * 2 + core, chip * 2 + 1 - core

    def load_a(i):
        slot = lax.rem(i, n_a)
        rows = pl.ds(pl.multiple_of(i // e_local * depth, depth), depth)
        e = lax.rem(i, e_local)
        return (pltpu.make_async_copy(wg_hbm.at[e, rows], wg.at[slot], s_w.at[0, slot]),
                pltpu.make_async_copy(wu_hbm.at[e, rows], wu.at[slot], s_w.at[1, slot]))

    def load_b(i):
        slot = lax.rem(i, n_b)
        q, g = i // groups, lax.rem(i, groups)
        cols = pl.ds(pl.multiple_of(q * wide, wide), wide)
        return pltpu.make_async_copy(wd_hbm.at[pl.ds(g * per, per), :, cols], wd.at[slot], s_d.at[slot])

    for e in range(n_a):
        for c in load_a(e):
            c.start()
    for i in range(n_b):
        load_b(i).start()

    barrier = pltpu.get_barrier_semaphore()
    for k in range(1, ep_size):
        pl.semaphore_signal(barrier, inc=1, device_id={'ep': lax.rem(me + k, ep_size)}, device_id_type=MESH)
    pl.semaphore_wait(barrier, ep_size - 1)

    def part(h):
        return pl.ds(h * half, half)

    def send_own(k, h, target, sem):
        cols = pl.ds(k * depth, depth)
        return pltpu.make_async_remote_copy(h_ref.at[part(h), cols], xall.at[k, me, part(h)], s_own.at[k, sem],
                                            r_x.at[k, me, h], device_id={'ep': target}, device_id_type=MESH)

    def forward(k, src, h, target, sem):
        return pltpu.make_async_remote_copy(xall.at[k, src, part(h)], xall.at[k, src, part(h)], s_fwd.at[k, sem],
                                            r_x.at[k, src, h], device_id={'ep': target}, device_id_type=MESH)

    def send_meta(k):
        return pltpu.make_async_remote_copy(meta_ref, mall.at[me], s_meta.at[k - 1], r_meta.at[me],
                                            device_id={'ep': lax.rem(me + k, ep_size)}, device_id_type=MESH)

    dev_f = far * 2 + core
    outgoing = ((0, dev_r), (1, dev_l), (1, dev_r), (0, dev_l), (0, mate), (1, mate))
    passed = ((dev_l, 0, dev_r), (dev_r, 1, dev_l), (dev_l, 0, mate), (dev_r, 1, mate))
    handed = ((dev_l, 1, mate), (dev_r, 0, mate), (dev_f, 0, mate), (dev_f, 1, mate))

    def own(k):
        for i, (h, target) in enumerate(outgoing):
            send_own(k, h, target, i).start()

    def pump(k):
        for i, (src, h, target) in enumerate(passed):
            if target is not mate:
                forward(k, src, h, target, i).wait_recv()
        for i, (src, h, target) in enumerate(passed):
            forward(k, src, h, target, i).start()

    def hand(k):
        for i, (src, h, target) in enumerate(handed):
            forward(k, src, h, target, 4 + i).wait_recv()
            forward(k, src, h, target, 4 + i).start()

    def arrive(k):
        for c in range(n_chip):
            src = lax.rem(chip + c, n_chip) * 2 + 1 - core
            for h in range(2):
                forward(k, src, h, mate, 0).wait_recv()

    for k in range(1, ep_size):
        send_meta(k).start()
    own(0)
    for k in range(DEEP):
        xall[k, me] = h_ref[:, k * depth:(k + 1) * depth]
    mall[me] = meta_ref[...]
    pump(0)
    own(1)

    for k in range(1, ep_size):
        src = lax.rem(me + k, ep_size)
        pltpu.make_async_remote_copy(meta_ref, mall.at[src], s_meta.at[k - 1], r_meta.at[src],
                                     device_id={'ep': src}, device_id_type=MESH).wait_recv()
    lower = lax.broadcasted_iota(jnp.int32, (b_dev, b_dev), 0) < lax.broadcasted_iota(jnp.int32, (b_dev, b_dev), 1)
    before = jnp.where(lower, 1.0, 0.0).astype(BF16)
    ids16 = lax.broadcasted_iota(jnp.int32, (e_local, b_dev), 0).astype(F32)
    keys[...] = jnp.zeros_like(keys)
    counts = jnp.zeros((e_local, 1), F32)
    for src in range(ep_size):
        row = mall[src, pl.ds(me, 1), :]
        hot = jnp.where(ids16 == row, 1.0, 0.0)
        ranks = jnp.dot(hot.astype(BF16), before, preferred_element_type=F32) + counts
        rank = jnp.sum(hot * ranks, axis=0, keepdims=True)
        keys[pl.ds(src, 1), :] = row * SEATS + rank
        keys[pl.ds(ep_size + src, 1), :] = mall[src, pl.ds(ep_size + me, 1), :]
        keys[pl.ds(2 * ep_size + src, 1), :] = mall[src, pl.ds(ep_size + mate, 1), :]
        counts = counts + jnp.sum(hot, axis=1, keepdims=True)
    keyt = jnp.transpose(keys[...])
    for b in range(2 * ep_size):
        share[b] = jnp.broadcast_to(keyt[:, ep_size + b:ep_size + b + 1], (b_dev, b_dev))
    most = jnp.zeros((e_local, 1), F32)
    for dev in range(ep_size):
        total = jnp.zeros((e_local, 1), F32)
        for src in range(ep_size):
            hot = jnp.where(ids16 == mall[src, pl.ds(dev, 1), :], 1.0, 0.0)
            total = total + jnp.sum(hot, axis=1, keepdims=True)
        most = jnp.maximum(most, total)
    flag_ref[0] = jnp.max(most)

    seat_cols = lax.broadcasted_iota(jnp.int32, (b_dev, 4 * SEATS), 1).astype(F32)
    for b in range(ep_size):
        col = jnp.transpose(keys[...])[:, b:b + 1]

        @pl.loop(0, e_local // 4)
        def _(j):
            base = (j * (4 * SEATS)).astype(F32)
            hot = jnp.where(seat_cols + base == col, 1.0, 0.0).astype(BF16)
            perm[b * b_dev:(b + 1) * b_dev, pl.ds(pl.multiple_of(j * (4 * SEATS), 4 * SEATS), 4 * SEATS)] = hot

    hand(0)
    arrive(0)

    seat_rows = lax.broadcasted_iota(jnp.int32, (SEATS, b_dev), 0).astype(F32)

    n_ff = ff // side

    def pick_rows(k, e, out):
        base = (e * SEATS).astype(F32)
        pick = jnp.concatenate(
            [jnp.where(keys[b:b + 1, :] == seat_rows + base, 1.0, 0.0).astype(BF16) for b in range(ep_size)], axis=1)
        for n in range(depth // 512):
            cols = slice(n * 512, (n + 1) * 512)
            rows = xall[k, :, :, cols].reshape(ep_size * b_dev, 512)
            out[:, cols] = jnp.dot(pick, rows, preferred_element_type=F32).astype(BF16)

    def project(k, e, rows):
        slot = lax.rem(k * e_local + e, n_a)
        for n in range(n_ff):
            cols = slice(n * side, (n + 1) * side)
            gate = jnp.dot(rows[...], wg[slot, :, cols], preferred_element_type=F32)
            up = jnp.dot(rows[...], wu[slot, :, cols], preferred_element_type=F32)
            at = e * (2 * n_ff) + 2 * n
            if k:
                gate = gate + acc[at]
                up = up + acc[at + 1]
            if k < DEEP - 1:
                acc[at] = gate
                acc[at + 1] = up
            else:
                hid[e, :, cols] = (gate * jax.nn.sigmoid(gate) * up).astype(BF16)

    def refill(item):
        @pl.when(item + n_a < DEEP * e_local)
        def _():
            for c in load_a(item + n_a):
                c.start()

    def down(q, g):
        i = q * groups + g
        slot = lax.rem(i, n_b)
        load_b(i).wait()
        for j in range(per):
            e = g * per + j
            ys[pl.ds(pl.multiple_of(e * SEATS, SEATS), SEATS), :] = jnp.dot(
                hid[e], wd[slot, j], preferred_element_type=F32).astype(BF16)

        @pl.when(i + n_b < SPLIT * groups)
        def _():
            load_b(i + n_b).start()

    for k in range(DEEP):
        pick_rows(k, jnp.int32(0), xg_even)

        @pl.loop(0, e_local // 2)
        def _(p):
            for odd, (now, later) in enumerate(((xg_even, xg_odd), (xg_odd, xg_even))):
                e = 2 * p + odd
                for c in load_a(k * e_local + e):
                    c.wait()
                pick_rows(k, jnp.minimum(e + 1, e_local - 1), later)
                project(k, e, now)
                refill(k * e_local + e)
            if k + 1 < DEEP:
                @pl.when(p == 0)
                def _():
                    pump(k + 1)
                    if k + 2 < DEEP:
                        own(k + 2)

                @pl.when(p == 3)
                def _():
                    hand(k + 1)
            else:
                @pl.when(lax.rem(p, per // 2) == per // 2 - 1)
                def _():
                    down(0, p // (per // 2))

        if k + 1 < DEEP:
            arrive(k + 1)

    def chip_of(m):
        return lax.rem(chip + 2 + m, n_chip)

    def send_y(q, m):
        blocks = pl.ds(2 * chip_of(m), 2)
        return pltpu.make_async_remote_copy(ybuf.at[lax.rem(q, 2), 1 - core, blocks], yrecv.at[q, blocks],
                                            s_y.at[q, m], r_y.at[q, m], device_id={'ep': mate}, device_id_type=MESH)

    def send_1(q, d):
        block = far * 2 + d
        return pltpu.make_async_remote_copy(acc.at[q * ep_size + block], recv1.at[d, q], s_1.at[d, q], r_1.at[d, q],
                                            device_id={'ep': dev_l if d else dev_r}, device_id_type=MESH)

    def send_2(q, d):
        block = (left if d else right) * 2
        return pltpu.make_async_remote_copy(acc.at[pl.ds(q * ep_size + block, 2)], recv2.at[d, q], s_2.at[d, q], r_2.at[d, q],
                                            device_id={'ep': dev_l if d else dev_r}, device_id_type=MESH)

    def send_f(q):
        return pltpu.make_async_remote_copy(acc.at[q * ep_size + mate], fin.at[q], s_f.at[q], r_f.at[q],
                                            device_id={'ep': mate}, device_id_type=MESH)

    def relay(q):
        for d in range(2):
            send_1(q, d).wait_recv()
            block = (left if d else right) * 2 + d
            acc[q * ep_size + block] = acc[q * ep_size + block] + recv1[d, q]
            send_2(q, d).start()

    def weigh(q, m):
        send_y(q, m).wait_recv()
        for j in range(2):
            b = 2 * chip_of(m) + j
            for n in range(side // b_dev):
                cols = slice(n * b_dev, (n + 1) * b_dev)
                acc[q * ep_size + b, :, cols] = (share[b] * ybuf[lax.rem(q, 2), core, b, :, cols].astype(F32)
                                                 + share[ep_size + b] * yrecv[q, b, :, cols].astype(F32))

    @pl.loop(0, SPLIT)
    def _(q):
        @pl.when(q > 0)
        def _():
            @pl.loop(0, groups)
            def _(g):
                down(q, g)

        @pl.when(q > 1)
        def _():
            for m in range(n_chip):
                send_y(q - 2, m).wait_send()

        @pl.loop(0, n_chip)
        def _(m):
            rows = pl.ds(pl.multiple_of(chip_of(m) * (2 * b_dev), 2 * b_dev), 2 * b_dev)
            back = jnp.dot(perm[rows, :], ys[...], preferred_element_type=F32).astype(BF16)
            for h in range(2):
                ybuf[lax.rem(q, 2), h, pl.ds(2 * chip_of(m), 2)] = back[:, h * side:(h + 1) * side].reshape(2, b_dev, side)
            send_y(q, m).start()

        weigh(q, 0)
        send_1(q, 0).start()
        send_1(q, 1).start()

        @pl.when(q > 0)
        def _():
            relay(q - 1)

        for m in range(1, n_chip):
            weigh(q, m)

    relay(SPLIT - 1)

    def columns(q, which):
        return pl.ds(pl.multiple_of(q * wide + which * side, side), side)

    @pl.loop(0, SPLIT)
    def _(q):
        send_2(q, 0).wait_recv()
        send_2(q, 1).wait_recv()
        acc[q * ep_size + mate] = acc[q * ep_size + mate] + recv2[0, q, 1 - core] + recv2[1, q, 1 - core]
        send_f(q).start()
        mine = acc[q * ep_size + me] + recv2[0, q, core] + recv2[1, q, core]
        cols = columns(q, core)
        out_ref[:, cols] = (x_ref[:, cols].astype(F32) + mine).astype(BF16)

    @pl.loop(0, SPLIT)
    def _(q):
        send_f(q).wait_recv()
        cols = columns(q, 1 - core)
        out_ref[:, cols] = (x_ref[:, cols].astype(F32) + fin[q]).astype(BF16)

    for k in range(1, ep_size):
        send_meta(k).wait_send()
    for k in range(DEEP):
        for i, (h, target) in enumerate(outgoing):
            send_own(k, h, target, i).wait_send()
        for i, (src, h, target) in enumerate(passed + handed):
            forward(k, src, h, target, i).wait_send()

    @pl.loop(0, SPLIT)
    def _(q):
        @pl.when(q >= SPLIT - 2)
        def _():
            for m in range(n_chip):
                send_y(q, m).wait_send()

        send_f(q).wait_send()
        for d in range(2):
            send_1(q, d).wait_send()
            send_2(q, d).wait_send()


def moe_block(ep_size, h_moe, x_mid, meta, w_gate, w_up, w_down):
    b_dev, hidden = h_moe.shape
    e_local, _, ff = w_gate.shape
    wide, side = hidden // SPLIT, hidden // SPLIT // 2
    n_a, n_b, per = 4, 3, 4
    depth, n_ff = hidden // DEEP, ff // side
    vmem, dma = pltpu.VMEM, pltpu.SemaphoreType.DMA
    tokens = ep_size * b_dev
    return pl.pallas_call(
        functools.partial(moe_kernel, ep_size),
        out_shape=(jax.ShapeDtypeStruct((b_dev, hidden), BF16), jax.ShapeDtypeStruct((1,), F32)),
        in_specs=[pl.BlockSpec(memory_space=pltpu.VMEM)] * 3 + [pl.BlockSpec(memory_space=pl.ANY)] * 3,
        out_specs=(pl.BlockSpec(memory_space=pltpu.VMEM), pl.BlockSpec(memory_space=pltpu.SMEM)),
        scratch_shapes=[
            vmem((DEEP, ep_size, b_dev, depth), BF16), vmem((ep_size, 2 * ep_size, b_dev), F32),
            vmem((tokens, e_local * SEATS), BF16), vmem((b_dev, b_dev), F32), vmem((2 * ep_size, b_dev, b_dev), F32),
            vmem((SEATS, depth), BF16), vmem((SEATS, depth), BF16), vmem((e_local, SEATS, ff), BF16), vmem((e_local * SEATS, wide), BF16),
            vmem((2, 2, ep_size, b_dev, side), BF16), vmem((SPLIT, ep_size, b_dev, side), BF16),
            vmem((max(e_local * 2 * n_ff, SPLIT * ep_size), b_dev, side), F32), vmem((2, SPLIT, b_dev, side), F32),
            vmem((2, SPLIT, 2, b_dev, side), F32), vmem((SPLIT, b_dev, side), F32),
            vmem((n_a, depth, ff), BF16), vmem((n_a, depth, ff), BF16), vmem((n_b, per, ff, wide), BF16),
            dma((2, n_a)), dma((n_b,)), dma((DEEP, 6)), dma((DEEP, 8)), dma((DEEP, ep_size, 2)),
            dma((ep_size - 1,)), dma((ep_size,)),
            dma((SPLIT, ep_size // 2)), dma((SPLIT, ep_size // 2)), dma((2, SPLIT)), dma((2, SPLIT)), dma((2, SPLIT)), dma((2, SPLIT)),
            dma((SPLIT,)), dma((SPLIT,)),
        ],
        compiler_params=pltpu.CompilerParams(collective_id=0, has_side_effects=True, vmem_limit_bytes=67043328),
        name='moe',
    )(h_moe, x_mid, meta, w_gate, w_up, w_down)


def moe_general(ep_size, h_moe, x_mid, meta, w_gate, w_up, w_down):
    b_dev, hidden = h_moe.shape
    rows = lax.all_to_all(jnp.broadcast_to(h_moe[None], (ep_size, b_dev, hidden)), 'ep', 0, 0, tiled=True)
    rows = rows.reshape(ep_size * b_dev, hidden)
    ids = lax.all_to_all(meta[:ep_size, None, :], 'ep', 0, 0, tiled=True).reshape(ep_size * b_dev)

    def one(e, done):
        gate = jnp.dot(rows, w_gate[e], preferred_element_type=F32)
        up = jnp.dot(rows, w_up[e], preferred_element_type=F32)
        act = (jax.nn.silu(gate) * up).astype(BF16)
        y = jnp.dot(act, w_down[e], preferred_element_type=F32).astype(BF16)
        return jnp.where((ids == e.astype(F32))[:, None], y, done)

    y = lax.fori_loop(0, w_gate.shape[0], one, jnp.zeros(rows.shape, BF16))
    back = lax.all_to_all(y.reshape(ep_size, b_dev, hidden), 'ep', 0, 0, tiled=True)
    total = jnp.sum(back.astype(F32) * meta[ep_size:, :, None], axis=0)
    return (x_mid.astype(F32) + total).astype(BF16)


def solution(mesh):
    ep_size = mesh.shape['ep']
    row_spec = P(('dp', 'ep'))
    replicated = P()
    expert_spec = P('ep')
    in_specs = (row_spec,) * 5 + (replicated,) * 9 + (expert_spec,) * 3
    out_specs = (row_spec, row_spec, row_spec)

    def device_step(x_in, k_cache, v_cache, cache_len, topk_idx, ln_attn, w_q, w_k, w_v, q_norm, k_norm, w_o, ln_moe, w_router, w_gate, w_up, w_down):
        x_mid, h_moe, meta, k_full, v_full = attend_block(
            ep_size, x_in, k_cache, v_cache, cache_len, topk_idx, ln_attn, w_q, w_k, w_v, q_norm, k_norm, w_o, ln_moe, w_router)
        fast, most = moe_block(ep_size, h_moe, x_mid, meta, w_gate, w_up, w_down)
        x_out = lax.while_loop(
            lambda state: state[0][0] > SEATS,
            lambda state: (jnp.zeros_like(state[0]), moe_general(ep_size, h_moe, x_mid, meta, w_gate, w_up, w_down)),
            (most, fast))[1]
        return x_out, k_full, v_full

    return jax.shard_map(device_step, mesh=mesh, in_specs=in_specs, out_specs=out_specs, check_vma=False)
```

```python
import functools
import math

import jax
import jax.numpy as jnp
from jax import lax
from jax.experimental import pallas as pl
from jax.experimental.pallas import tpu as pltpu
from jax.sharding import PartitionSpec as P

ROPE_BASE = 1000000.0
NORM_EPS = 1e-6
MESH = pl.DeviceIdType.MESH
F32 = jnp.float32
BF16 = jnp.bfloat16
SEATS = 128
SPLIT = 4
DEEP = 2


def rms(values):
    return values * lax.rsqrt(jnp.mean(values * values, axis=-1, keepdims=True) + NORM_EPS)


def rms_rows(values, gain_ref, out_ref):
    normed = rms(values)
    lanes = gain_ref.shape[1]
    for i in range(gain_ref.shape[0]):
        cols = slice(i * lanes, (i + 1) * lanes)
        out_ref[:, cols] = (normed[:, cols] * gain_ref[i:i + 1, :].astype(F32)).astype(BF16)


def attend_kernel(ep_size, len_ref, x_ref, row_ref, idx_ref, lna_ref, qn_ref, kn_ref, lnm_ref,
                  wq_hbm, wk_hbm, wv_hbm, wo_hbm, wr_hbm, kc_hbm, vc_hbm,
                  xmid_ref, h_ref, meta_ref, ko_hbm, vo_hbm,
                  wq, wk, wv, wo, wr, kbuf, vbuf, qs, os, knew, vnew, hn, att, part,
                  s_q, s_kv, s_o, s_c, s_out):
    b_dev, hidden = x_ref.shape
    _, lanes, dim = kbuf.shape
    q_width = wq.shape[1]
    q_heads, kv_heads = q_width // dim, wk.shape[1] // dim
    n_q, n_o = s_q.shape[0], s_o.shape[0]
    n_blk = s_c.shape[1]
    blk = b_dev // n_blk
    deep, qc, oc = hidden // n_q, part.shape[2], hidden // 2
    n_part = q_width // qc
    rep = q_heads // kv_heads

    def copy_q(i):
        rows = pl.ds(i * deep, deep)
        return pltpu.make_async_copy(wq_hbm.at[rows], wq.at[rows], s_q.at[i])

    def copy_o(i):
        rows = pl.ds(i * (q_width // n_o), q_width // n_o)
        return pltpu.make_async_copy(wo_hbm.at[rows], wo.at[rows], s_o.at[i])

    def copy_in(b):
        rows = pl.ds(b * blk, blk)
        return (pltpu.make_async_copy(kc_hbm.at[rows], kbuf.at[rows], s_c.at[0, b]),
                pltpu.make_async_copy(vc_hbm.at[rows], vbuf.at[rows], s_c.at[1, b]))

    def copy_out(b):
        rows = pl.ds(b * blk, blk)
        return (pltpu.make_async_copy(kbuf.at[rows], ko_hbm.at[rows], s_out.at[0, b]),
                pltpu.make_async_copy(vbuf.at[rows], vo_hbm.at[rows], s_out.at[1, b]))

    small = (pltpu.make_async_copy(wk_hbm, wk, s_kv.at[0]), pltpu.make_async_copy(wv_hbm, wv, s_kv.at[1]),
             pltpu.make_async_copy(wr_hbm, wr, s_kv.at[2]))
    for c in small[:2]:
        c.start()
    for i in range(n_q):
        copy_q(i).start()
    for b in range(n_blk):
        for c in copy_in(b):
            c.start()

    x = x_ref[...].astype(F32)
    rms_rows(x, lna_ref, hn)
    pair = lax.rem(lax.broadcasted_iota(jnp.int32, (b_dev, dim), 1), dim // 2).astype(F32)
    freq = jnp.exp(pair * (-2.0 / dim * math.log(ROPE_BASE)))
    angle = jnp.transpose(jnp.broadcast_to(row_ref[...].astype(F32), (dim, b_dev))) * freq
    cos = jnp.cos(angle)
    sin = jnp.where(lax.broadcasted_iota(jnp.int32, (b_dev, dim), 1) < dim // 2, -1.0, 1.0) * jnp.sin(angle)

    def turned(values, gain):
        normed = rms(values) * gain
        return (normed * cos + pltpu.roll(normed, dim // 2, 1) * sin).astype(BF16).astype(F32)

    small[0].wait()
    small[1].wait()
    key = jnp.dot(hn[...], wk[...], preferred_element_type=F32)
    val = jnp.dot(hn[...], wv[...], preferred_element_type=F32).astype(BF16).astype(F32)
    for g in range(kv_heads):
        cols = slice(g * dim, (g + 1) * dim)
        turned_k = turned(key[:, cols], kn_ref[...].astype(F32))
        for r in range(8 // kv_heads):
            rows = pl.ds(g + kv_heads * r, b_dev, stride=8)
            knew[rows, :] = turned_k
            vnew[rows, :] = val[:, cols]
    def spread(i):
        for j in range(qc // dim):
            qs[pl.ds(i * (qc // dim) + j, b_dev, stride=q_heads), :] = turned(
                part[i % 2, :, j * dim:(j + 1) * dim], qn_ref[...].astype(F32))

    for i in range(n_q):
        copy_q(i).wait()
    for i in range(n_o):
        copy_o(i).start()
    small[2].start()
    for i in range(n_part):
        part[i % 2] = jnp.dot(hn[...], wq[:, i * qc:(i + 1) * qc], preferred_element_type=F32)
        if i:
            spread(i - 1)
    spread(n_part - 1)

    row_slot = lax.broadcasted_iota(jnp.int32, (lanes, dim), 0) // kv_heads
    lane = lax.broadcasted_iota(jnp.int32, (q_heads, lanes), 1)
    own_head = lax.rem(lane, kv_heads) == lax.broadcasted_iota(jnp.int32, (q_heads, lanes), 0) // rep
    lane_slot = jnp.where(own_head, lane // kv_heads, lanes)

    @pl.loop(0, n_blk)
    def _(b):
        for c in copy_in(b):
            c.wait()
        scores = []
        for j in range(blk):
            t = b * blk + j
            size = len_ref[t]
            here = row_slot == size
            fresh = pl.ds(pl.multiple_of(t * 8, 8), 8)
            k_row = jnp.concatenate([knew[fresh, :]] * (lanes // 8), axis=0)
            v_row = jnp.concatenate([vnew[fresh, :]] * (lanes // 8), axis=0)
            k_tok = jnp.where(here, k_row, kbuf[t].astype(F32)).astype(BF16)
            kbuf[t] = k_tok
            vbuf[t] = jnp.where(here, v_row, vbuf[t].astype(F32)).astype(BF16)
            q_tok = qs[pl.ds(pl.multiple_of(t * q_heads, q_heads), q_heads), :].astype(BF16)
            score = lax.dot_general(q_tok, k_tok, (((1,), (1,)), ((), ())), preferred_element_type=F32)
            scores.append(jnp.where(lane_slot <= size, score * dim ** -0.5, -1e30))
        score = jnp.concatenate(scores, axis=0)
        weight = jnp.exp(score - jnp.max(score, axis=1, keepdims=True))
        prob = (weight / jnp.sum(weight, axis=1, keepdims=True)).astype(BF16)
        for j in range(blk):
            t = b * blk + j
            os[pl.ds(pl.multiple_of(t * q_heads, q_heads), q_heads), :] = jnp.dot(
                prob[j * q_heads:(j + 1) * q_heads, :], vbuf[t], preferred_element_type=F32)
        for c in copy_out(b):
            c.start()

    for h in range(q_heads):
        att[:, h * dim:(h + 1) * dim] = os[pl.ds(h, b_dev, stride=q_heads), :].astype(BF16)
    for i in range(n_o):
        copy_o(i).wait()
    for i in range(hidden // oc):
        cols = slice(i * oc, (i + 1) * oc)
        out = jnp.dot(att[...], wo[:, cols], preferred_element_type=F32)
        xmid_ref[:, cols] = (x_ref[:, cols].astype(F32) + out).astype(BF16)
    rms_rows(xmid_ref[...].astype(F32), lnm_ref, h_ref)
    small[2].wait()
    logits = jnp.transpose(jnp.dot(h_ref[...], wr[...], preferred_element_type=F32))
    experts = logits.shape[0]
    e_local = experts // ep_size
    expert = lax.broadcasted_iota(jnp.int32, (experts, b_dev), 0)
    chosen = expert == idx_ref[0:1, :]
    for k in range(1, idx_ref.shape[0]):
        chosen = chosen | (expert == idx_ref[k:k + 1, :])
    top = jnp.max(jnp.where(chosen, logits, -1e30), axis=0, keepdims=True)
    mass = jnp.where(chosen, jnp.exp(logits - top), 0.0)
    mass = mass / jnp.sum(mass, axis=0, keepdims=True)
    local = jnp.where(chosen, lax.rem(expert, e_local), 0).astype(F32)
    meta_ref[0:ep_size, :] = jnp.sum(local.reshape(ep_size, e_local, b_dev), axis=1)
    meta_ref[ep_size:2 * ep_size, :] = jnp.sum(mass.reshape(ep_size, e_local, b_dev), axis=1)

    for b in range(n_blk):
        for c in copy_out(b):
            c.wait()


def attend_block(ep_size, x_in, k_cache, v_cache, cache_len, topk_idx, ln_attn, w_q, w_k, w_v, q_norm, k_norm, w_o, ln_moe, w_router):
    b_dev, hidden = x_in.shape
    _, n_slots, kv_heads, dim = k_cache.shape
    q_width, kv_width, experts = w_q.shape[1], w_k.shape[1], w_router.shape[1]
    q_heads = q_width // dim
    lanes = n_slots * kv_heads
    n_q, n_o, n_blk = 8, 4, 2
    vmem, dma, far = pltpu.VMEM, pltpu.SemaphoreType.DMA, pl.BlockSpec(memory_space=pl.ANY)
    near = pl.BlockSpec(memory_space=pltpu.VMEM)
    flat = (b_dev, lanes, dim)
    x_mid, h_moe, meta, k_new, v_new = pl.pallas_call(
        functools.partial(attend_kernel, ep_size),
        out_shape=(jax.ShapeDtypeStruct((b_dev, hidden), BF16), jax.ShapeDtypeStruct((b_dev, hidden), BF16),
                   jax.ShapeDtypeStruct((2 * ep_size, b_dev), F32),
                   jax.ShapeDtypeStruct(flat, BF16), jax.ShapeDtypeStruct(flat, BF16)),
        in_specs=[pl.BlockSpec(memory_space=pltpu.SMEM)] + [near] * 7 + [far] * 7,
        out_specs=(near, near, near, far, far),
        scratch_shapes=[
            vmem((hidden, q_width), BF16), vmem((hidden, kv_width), BF16), vmem((hidden, kv_width), BF16),
            vmem((q_width, hidden), BF16), vmem((hidden, experts), BF16), vmem(flat, BF16), vmem(flat, BF16),
            vmem((b_dev * q_heads, dim), F32), vmem((b_dev * q_heads, dim), F32),
            vmem((b_dev * 8, dim), F32), vmem((b_dev * 8, dim), F32),
            vmem((b_dev, hidden), BF16), vmem((b_dev, q_width), BF16), vmem((2, b_dev, q_width // 8), F32),
            dma((n_q,)), dma((3,)), dma((n_o,)), dma((2, n_blk)), dma((2, n_blk)),
        ],
        compiler_params=pltpu.CompilerParams(vmem_limit_bytes=67043328),
        name='attend',
    )(cache_len, x_in, cache_len[None], topk_idx.T, ln_attn.reshape(-1, dim), q_norm[None], k_norm[None], ln_moe.reshape(-1, dim),
      w_q, w_k, w_v, w_o, w_router, k_cache.reshape(flat), v_cache.reshape(flat))
    return x_mid, h_moe, meta, k_new.reshape(k_cache.shape), v_new.reshape(v_cache.shape)


def moe_kernel(ep_size, h_ref, x_ref, meta_ref, wg_hbm, wu_hbm, wd_hbm, out_ref, flag_ref,
               xall, mall, perm, keys, share, xg_even, xg_odd, hid, ys, ybuf, yrecv, acc, recv1, recv2, fin,
               wg, wu, wd, s_w, s_d, s_own, s_fwd, r_x, s_meta, r_meta,
               s_y, r_y, s_1, r_1, s_2, r_2, s_f, r_f):
    b_dev, hidden = h_ref.shape
    e_local, _, ff = wg_hbm.shape
    n_chip = ep_size // 2
    half = b_dev // 2
    depth = hidden // DEEP
    wide = hidden // SPLIT
    side = wide // 2
    n_a, n_b = wg.shape[0], wd.shape[0]
    per = wd.shape[1]
    groups = e_local // per
    me = lax.axis_index('ep')
    chip, core = me // 2, me % 2
    right = lax.rem(chip + 1, n_chip)
    left = lax.rem(chip + n_chip - 1, n_chip)
    far = lax.rem(chip + 2, n_chip)
    dev_r, dev_l, mate = right * 2 + core, left * 2 + core, chip * 2 + 1 - core

    def load_a(i):
        slot = lax.rem(i, n_a)
        rows = pl.ds(pl.multiple_of(i // e_local * depth, depth), depth)
        e = lax.rem(i, e_local)
        return (pltpu.make_async_copy(wg_hbm.at[e, rows], wg.at[slot], s_w.at[0, slot]),
                pltpu.make_async_copy(wu_hbm.at[e, rows], wu.at[slot], s_w.at[1, slot]))

    def load_b(i):
        slot = lax.rem(i, n_b)
        q, g = i // groups, lax.rem(i, groups)
        cols = pl.ds(pl.multiple_of(q * wide, wide), wide)
        return pltpu.make_async_copy(wd_hbm.at[pl.ds(g * per, per), :, cols], wd.at[slot], s_d.at[slot])

    for e in range(n_a):
        for c in load_a(e):
            c.start()
    for i in range(n_b):
        load_b(i).start()

    barrier = pltpu.get_barrier_semaphore()
    for k in range(1, ep_size):
        pl.semaphore_signal(barrier, inc=1, device_id={'ep': lax.rem(me + k, ep_size)}, device_id_type=MESH)
    pl.semaphore_wait(barrier, ep_size - 1)

    def part(h):
        return pl.ds(h * half, half)

    def send_own(k, h, target, sem):
        cols = pl.ds(k * depth, depth)
        return pltpu.make_async_remote_copy(h_ref.at[part(h), cols], xall.at[k, me, part(h)], s_own.at[k, sem],
                                            r_x.at[k, me, h], device_id={'ep': target}, device_id_type=MESH)

    def forward(k, src, h, target, sem):
        return pltpu.make_async_remote_copy(xall.at[k, src, part(h)], xall.at[k, src, part(h)], s_fwd.at[k, sem],
                                            r_x.at[k, src, h], device_id={'ep': target}, device_id_type=MESH)

    def send_meta(k):
        return pltpu.make_async_remote_copy(meta_ref, mall.at[me], s_meta.at[k - 1], r_meta.at[me],
                                            device_id={'ep': lax.rem(me + k, ep_size)}, device_id_type=MESH)

    dev_f = far * 2 + core
    outgoing = ((0, dev_r), (1, dev_l), (1, dev_r), (0, dev_l), (0, mate), (1, mate))
    passed = ((dev_l, 0, dev_r), (dev_r, 1, dev_l), (dev_l, 0, mate), (dev_r, 1, mate))
    handed = ((dev_l, 1, mate), (dev_r, 0, mate), (dev_f, 0, mate), (dev_f, 1, mate))

    def own(k):
        for i, (h, target) in enumerate(outgoing):
            send_own(k, h, target, i).start()

    def pump(k):
        for i, (src, h, target) in enumerate(passed):
            if target is not mate:
                forward(k, src, h, target, i).wait_recv()
        for i, (src, h, target) in enumerate(passed):
            forward(k, src, h, target, i).start()

    def hand(k):
        for i, (src, h, target) in enumerate(handed):
            forward(k, src, h, target, 4 + i).wait_recv()
            forward(k, src, h, target, 4 + i).start()

    def arrive(k):
        for c in range(n_chip):
            src = lax.rem(chip + c, n_chip) * 2 + 1 - core
            for h in range(2):
                forward(k, src, h, mate, 0).wait_recv()

    for k in range(1, ep_size):
        send_meta(k).start()
    own(0)
    for k in range(DEEP):
        xall[k, me] = h_ref[:, k * depth:(k + 1) * depth]
    mall[me] = meta_ref[...]
    pump(0)
    own(1)

    for k in range(1, ep_size):
        src = lax.rem(me + k, ep_size)
        pltpu.make_async_remote_copy(meta_ref, mall.at[src], s_meta.at[k - 1], r_meta.at[src],
                                     device_id={'ep': src}, device_id_type=MESH).wait_recv()
    lower = lax.broadcasted_iota(jnp.int32, (b_dev, b_dev), 0) < lax.broadcasted_iota(jnp.int32, (b_dev, b_dev), 1)
    before = jnp.where(lower, 1.0, 0.0).astype(BF16)
    ids16 = lax.broadcasted_iota(jnp.int32, (e_local, b_dev), 0).astype(F32)
    keys[...] = jnp.zeros_like(keys)
    counts = jnp.zeros((e_local, 1), F32)
    for src in range(ep_size):
        row = mall[src, pl.ds(me, 1), :]
        hot = jnp.where(ids16 == row, 1.0, 0.0)
        ranks = jnp.dot(hot.astype(BF16), before, preferred_element_type=F32) + counts
        rank = jnp.sum(hot * ranks, axis=0, keepdims=True)
        keys[pl.ds(src, 1), :] = row * SEATS + rank
        keys[pl.ds(ep_size + src, 1), :] = mall[src, pl.ds(ep_size + me, 1), :]
        keys[pl.ds(2 * ep_size + src, 1), :] = mall[src, pl.ds(ep_size + mate, 1), :]
        counts = counts + jnp.sum(hot, axis=1, keepdims=True)
    keyt = jnp.transpose(keys[...])
    for b in range(2 * ep_size):
        share[b] = jnp.broadcast_to(keyt[:, ep_size + b:ep_size + b + 1], (b_dev, b_dev))
    most = jnp.zeros((e_local, 1), F32)
    for dev in range(ep_size):
        total = jnp.zeros((e_local, 1), F32)
        for src in range(ep_size):
            hot = jnp.where(ids16 == mall[src, pl.ds(dev, 1), :], 1.0, 0.0)
            total = total + jnp.sum(hot, axis=1, keepdims=True)
        most = jnp.maximum(most, total)
    flag_ref[0] = jnp.max(most)

    seat_cols = lax.broadcasted_iota(jnp.int32, (b_dev, 4 * SEATS), 1).astype(F32)
    for b in range(ep_size):
        col = keyt[:, b:b + 1]

        @pl.loop(0, e_local // 4)
        def _(j):
            base = (j * (4 * SEATS)).astype(F32)
            hot = jnp.where(seat_cols + base == col, 1.0, 0.0).astype(BF16)
            perm[b * b_dev:(b + 1) * b_dev, pl.ds(pl.multiple_of(j * (4 * SEATS), 4 * SEATS), 4 * SEATS)] = hot

    hand(0)
    arrive(0)

    seat_rows = lax.broadcasted_iota(jnp.int32, (SEATS, b_dev), 0).astype(F32)

    n_ff = ff // side

    def pick_rows(k, e, out):
        base = (e * SEATS).astype(F32)
        pick = jnp.concatenate(
            [jnp.where(keys[b:b + 1, :] == seat_rows + base, 1.0, 0.0).astype(BF16) for b in range(ep_size)], axis=1)
        for n in range(depth // 512):
            cols = slice(n * 512, (n + 1) * 512)
            rows = xall[k, :, :, cols].reshape(ep_size * b_dev, 512)
            out[:, cols] = jnp.dot(pick, rows, preferred_element_type=F32).astype(BF16)

    def project(k, e, rows):
        slot = lax.rem(k * e_local + e, n_a)
        for n in range(n_ff):
            cols = slice(n * side, (n + 1) * side)
            gate = jnp.dot(rows[...], wg[slot, :, cols], preferred_element_type=F32)
            up = jnp.dot(rows[...], wu[slot, :, cols], preferred_element_type=F32)
            at = e * (2 * n_ff) + 2 * n
            if k:
                gate = gate + acc[at]
                up = up + acc[at + 1]
            if k < DEEP - 1:
                acc[at] = gate
                acc[at + 1] = up
            else:
                hid[e, :, cols] = (gate * jax.nn.sigmoid(gate) * up).astype(BF16)

    def refill(item):
        @pl.when(item + n_a < DEEP * e_local)
        def _():
            for c in load_a(item + n_a):
                c.start()

    def down(q, g):
        i = q * groups + g
        slot = lax.rem(i, n_b)
        load_b(i).wait()
        for j in range(per):
            e = g * per + j
            ys[pl.ds(pl.multiple_of(e * SEATS, SEATS), SEATS), :] = jnp.dot(
                hid[e], wd[slot, j], preferred_element_type=F32).astype(BF16)

        @pl.when(i + n_b < SPLIT * groups)
        def _():
            load_b(i + n_b).start()

    for k in range(DEEP):
        pick_rows(k, jnp.int32(0), xg_even)

        @pl.loop(0, e_local // 2)
        def _(p):
            for odd, (now, later) in enumerate(((xg_even, xg_odd), (xg_odd, xg_even))):
                e = 2 * p + odd
                for c in load_a(k * e_local + e):
                    c.wait()
                pick_rows(k, jnp.minimum(e + 1, e_local - 1), later)
                project(k, e, now)
                refill(k * e_local + e)
            if k + 1 < DEEP:
                @pl.when(p == 1)
                def _():
                    pump(k + 1)
                    if k + 2 < DEEP:
                        own(k + 2)

                @pl.when(p == 4)
                def _():
                    hand(k + 1)
            else:
                @pl.when(lax.rem(p, per // 2) == per // 2 - 1)
                def _():
                    down(0, p // (per // 2))

        if k + 1 < DEEP:
            arrive(k + 1)

    def chip_of(m):
        return lax.rem(chip + 2 + m, n_chip)

    def send_y(q, m):
        blocks = pl.ds(2 * chip_of(m), 2)
        return pltpu.make_async_remote_copy(ybuf.at[lax.rem(q, 2), 1 - core, blocks], yrecv.at[q, blocks],
                                            s_y.at[q, m], r_y.at[q, m], device_id={'ep': mate}, device_id_type=MESH)

    def send_1(q, d):
        block = far * 2 + d
        return pltpu.make_async_remote_copy(acc.at[q * ep_size + block], recv1.at[d, q], s_1.at[d, q], r_1.at[d, q],
                                            device_id={'ep': dev_l if d else dev_r}, device_id_type=MESH)

    def send_2(q, d):
        block = (left if d else right) * 2
        return pltpu.make_async_remote_copy(acc.at[pl.ds(q * ep_size + block, 2)], recv2.at[d, q], s_2.at[d, q], r_2.at[d, q],
                                            device_id={'ep': dev_l if d else dev_r}, device_id_type=MESH)

    def send_f(q):
        return pltpu.make_async_remote_copy(acc.at[q * ep_size + mate], fin.at[q], s_f.at[q], r_f.at[q],
                                            device_id={'ep': mate}, device_id_type=MESH)

    def relay(q):
        for d in range(2):
            send_1(q, d).wait_recv()
            block = (left if d else right) * 2 + d
            acc[q * ep_size + block] = acc[q * ep_size + block] + recv1[d, q]
            send_2(q, d).start()

    def weigh(q, m):
        send_y(q, m).wait_recv()
        for j in range(2):
            b = 2 * chip_of(m) + j
            for n in range(side // b_dev):
                cols = slice(n * b_dev, (n + 1) * b_dev)
                acc[q * ep_size + b, :, cols] = (share[b] * ybuf[lax.rem(q, 2), core, b, :, cols].astype(F32)
                                                 + share[ep_size + b] * yrecv[q, b, :, cols].astype(F32))

    @pl.loop(0, SPLIT)
    def _(q):
        @pl.when(q > 0)
        def _():
            @pl.loop(0, groups)
            def _(g):
                down(q, g)

        @pl.when(q > 1)
        def _():
            for m in range(n_chip):
                send_y(q - 2, m).wait_send()

        @pl.loop(0, n_chip)
        def _(m):
            rows = pl.ds(pl.multiple_of(chip_of(m) * (2 * b_dev), 2 * b_dev), 2 * b_dev)
            back = jnp.dot(perm[rows, :], ys[...], preferred_element_type=F32).astype(BF16)
            for h in range(2):
                ybuf[lax.rem(q, 2), h, pl.ds(2 * chip_of(m), 2)] = back[:, h * side:(h + 1) * side].reshape(2, b_dev, side)
            send_y(q, m).start()

        weigh(q, 0)
        send_1(q, 0).start()
        send_1(q, 1).start()

        @pl.when(q > 0)
        def _():
            relay(q - 1)

        for m in range(1, n_chip):
            weigh(q, m)

    relay(SPLIT - 1)

    def columns(q, which):
        return pl.ds(pl.multiple_of(q * wide + which * side, side), side)

    @pl.loop(0, SPLIT)
    def _(q):
        send_2(q, 0).wait_recv()
        send_2(q, 1).wait_recv()
        acc[q * ep_size + mate] = acc[q * ep_size + mate] + recv2[0, q, 1 - core] + recv2[1, q, 1 - core]
        send_f(q).start()
        mine = acc[q * ep_size + me] + recv2[0, q, core] + recv2[1, q, core]
        cols = columns(q, core)
        out_ref[:, cols] = (x_ref[:, cols].astype(F32) + mine).astype(BF16)

    @pl.loop(0, SPLIT)
    def _(q):
        send_f(q).wait_recv()
        cols = columns(q, 1 - core)
        out_ref[:, cols] = (x_ref[:, cols].astype(F32) + fin[q]).astype(BF16)

    for k in range(1, ep_size):
        send_meta(k).wait_send()
    for k in range(DEEP):
        for i, (h, target) in enumerate(outgoing):
            send_own(k, h, target, i).wait_send()
        for i, (src, h, target) in enumerate(passed + handed):
            forward(k, src, h, target, i).wait_send()

    @pl.loop(0, SPLIT)
    def _(q):
        @pl.when(q >= SPLIT - 2)
        def _():
            for m in range(n_chip):
                send_y(q, m).wait_send()

        send_f(q).wait_send()
        for d in range(2):
            send_1(q, d).wait_send()
            send_2(q, d).wait_send()


def moe_block(ep_size, h_moe, x_mid, meta, w_gate, w_up, w_down):
    b_dev, hidden = h_moe.shape
    e_local, _, ff = w_gate.shape
    wide, side = hidden // SPLIT, hidden // SPLIT // 2
    n_a, n_b, per = 5, 3, 4
    depth, n_ff = hidden // DEEP, ff // side
    vmem, dma = pltpu.VMEM, pltpu.SemaphoreType.DMA
    tokens = ep_size * b_dev
    return pl.pallas_call(
        functools.partial(moe_kernel, ep_size),
        out_shape=(jax.ShapeDtypeStruct((b_dev, hidden), BF16), jax.ShapeDtypeStruct((1,), F32)),
        in_specs=[pl.BlockSpec(memory_space=pltpu.VMEM)] * 3 + [pl.BlockSpec(memory_space=pl.ANY)] * 3,
        out_specs=(pl.BlockSpec(memory_space=pltpu.VMEM), pl.BlockSpec(memory_space=pltpu.SMEM)),
        scratch_shapes=[
            vmem((DEEP, ep_size, b_dev, depth), BF16), vmem((ep_size, 2 * ep_size, b_dev), F32),
            vmem((tokens, e_local * SEATS), BF16), vmem((b_dev, b_dev), F32), vmem((2 * ep_size, b_dev, b_dev), F32),
            vmem((SEATS, depth), BF16), vmem((SEATS, depth), BF16), vmem((e_local, SEATS, ff), BF16), vmem((e_local * SEATS, wide), BF16),
            vmem((2, 2, ep_size, b_dev, side), BF16), vmem((SPLIT, ep_size, b_dev, side), BF16),
            vmem((max(e_local * 2 * n_ff, SPLIT * ep_size), b_dev, side), F32), vmem((2, SPLIT, b_dev, side), F32),
            vmem((2, SPLIT, 2, b_dev, side), F32), vmem((SPLIT, b_dev, side), F32),
            vmem((n_a, depth, ff), BF16), vmem((n_a, depth, ff), BF16), vmem((n_b, per, ff, wide), BF16),
            dma((2, n_a)), dma((n_b,)), dma((DEEP, 6)), dma((DEEP, 8)), dma((DEEP, ep_size, 2)),
            dma((ep_size - 1,)), dma((ep_size,)),
            dma((SPLIT, ep_size // 2)), dma((SPLIT, ep_size // 2)), dma((2, SPLIT)), dma((2, SPLIT)), dma((2, SPLIT)), dma((2, SPLIT)),
            dma((SPLIT,)), dma((SPLIT,)),
        ],
        compiler_params=pltpu.CompilerParams(collective_id=0, has_side_effects=True, vmem_limit_bytes=67043328),
        name='moe',
    )(h_moe, x_mid, meta, w_gate, w_up, w_down)


def moe_general(ep_size, h_moe, x_mid, meta, w_gate, w_up, w_down):
    b_dev, hidden = h_moe.shape
    rows = lax.all_to_all(jnp.broadcast_to(h_moe[None], (ep_size, b_dev, hidden)), 'ep', 0, 0, tiled=True)
    rows = rows.reshape(ep_size * b_dev, hidden)
    ids = lax.all_to_all(meta[:ep_size, None, :], 'ep', 0, 0, tiled=True).reshape(ep_size * b_dev)

    def one(e, done):
        gate = jnp.dot(rows, w_gate[e], preferred_element_type=F32)
        up = jnp.dot(rows, w_up[e], preferred_element_type=F32)
        act = (jax.nn.silu(gate) * up).astype(BF16)
        y = jnp.dot(act, w_down[e], preferred_element_type=F32).astype(BF16)
        return jnp.where((ids == e.astype(F32))[:, None], y, done)

    y = lax.fori_loop(0, w_gate.shape[0], one, jnp.zeros(rows.shape, BF16))
    back = lax.all_to_all(y.reshape(ep_size, b_dev, hidden), 'ep', 0, 0, tiled=True)
    total = jnp.sum(back.astype(F32) * meta[ep_size:, :, None], axis=0)
    return (x_mid.astype(F32) + total).astype(BF16)


def solution(mesh):
    ep_size = mesh.shape['ep']
    row_spec = P(('dp', 'ep'))
    replicated = P()
    expert_spec = P('ep')
    in_specs = (row_spec,) * 5 + (replicated,) * 9 + (expert_spec,) * 3
    out_specs = (row_spec, row_spec, row_spec)

    def device_step(x_in, k_cache, v_cache, cache_len, topk_idx, ln_attn, w_q, w_k, w_v, q_norm, k_norm, w_o, ln_moe, w_router, w_gate, w_up, w_down):
        x_mid, h_moe, meta, k_full, v_full = attend_block(
            ep_size, x_in, k_cache, v_cache, cache_len, topk_idx, ln_attn, w_q, w_k, w_v, q_norm, k_norm, w_o, ln_moe, w_router)
        fast, most = moe_block(ep_size, h_moe, x_mid, meta, w_gate, w_up, w_down)
        x_out = lax.while_loop(
            lambda state: state[0][0] > SEATS,
            lambda state: (jnp.zeros_like(state[0]), moe_general(ep_size, h_moe, x_mid, meta, w_gate, w_up, w_down)),
            (most, fast))[1]
        return x_out, k_full, v_full

    return jax.shard_map(device_step, mesh=mesh, in_specs=in_specs, out_specs=out_specs, check_vma=False)
```
